512 devices in a mesh: dp: 16 (over z, y_lo), comp: 32 (over y_hi, x, core).
Axes of the slice: x: 4, y: 8 (y_hi: 4, y_lo: 2; y = y_hi * 2 + y_lo), z: 8, core: 2. Of those that a mesh axis runs over, the one named last changes fastest.
Arguments:
- vectors: bfloat16 [2048, 256], P('dp'), may hold values from -8 to 8
- centers: float32 [512, 256], P('comp'), may hold values from -1.5 to 1.5
- factors: bfloat16 [512, 256, 256], P('comp', 'dp'), may hold values from -1 to 9.065873, as said below
- mixing: float32 [512], P('comp'), may hold values from 0.0005859375 to 0.005859375
Outputs:
- new_factors: float32 [512, 256, 256], P('comp', 'dp')
- new_means: float32 [512, 256], P('comp')
- new_weights: float32 [512], P('comp')
- evidence: float32 [2048], P('dp')
The draws below stay inside these ranges and needn't reach their ends.
Inputs may be any that keep to these rules, and one draw needn't show every extreme that they name: `factors`: each component's 256 x 256 factor is lower triangular with a positive diagonal.
All inputs are finite; a program needn't handle non-finite values.
Results may differ from the reference program's by a relative error of at most 0.0003.
Values may be sent and summed in bfloat16 or wider, within the bound.
No kernel may reach another device: no remote copies, remote signals or barrier semaphores. Data moves between devices by JAX's collectives and lax.ppermute only.
A program may use at most 64 MiB of HBM per device.

```python
import math
import jax
import jax.numpy as jnp
from jax import lax

D = 256
VECTORS = 2048
COMPONENTS = 512


def sharp_plan(key):
    plan_key = jax.random.fold_in(key, 71)
    picked = jax.random.permutation(plan_key, COMPONENTS)[:8]
    chosen = jax.random.permutation(jax.random.fold_in(plan_key, 1), VECTORS)[:4]
    return (picked, chosen)


def base_centers(key):
    center_key = jax.random.fold_in(key, 37)
    values = jnp.clip(jax.random.normal(center_key, (COMPONENTS, D)) * 0.5, -1.5, 1.5)
    picked, chosen = sharp_plan(key)
    values = values.at[picked[1::2]].set(values[picked[0::2]])
    return values.astype(jnp.float32)


def draw_centers(key, part):
    return base_centers(key)


def draw_vectors(key, part):
    first_key = jax.random.fold_in(jax.random.fold_in(key, 11), 0)
    values = jnp.clip(jax.random.normal(first_key, (VECTORS, D)), -5.0, 5.0)
    picked, chosen = sharp_plan(key)
    values = values.at[chosen].set(base_centers(key)[picked[0::2]])
    return values.astype(jnp.float32).astype(jnp.bfloat16)


def draw_factors(key, part):
    first_key, second_key = jax.random.split(jax.random.fold_in(key, 23))
    diag_lo, diag_hi, spread = (0.6, 1.6, 0.25)
    diagonal = jnp.exp(jax.random.uniform(first_key, (COMPONENTS, D), minval=math.log(diag_lo), maxval=math.log(diag_hi)))
    picked, chosen = sharp_plan(key)
    strength = jnp.array([1.0, 1.0, 1.2, 1.2, 1.4, 1.4, 1.0, 1.0], jnp.float32)
    log_sharp = jnp.broadcast_to((1.0 + 220.0 / D * strength)[:, None], (8, D))
    log_sharp = log_sharp.at[1::2, 0].add(-2.0)
    diagonal = diagonal.at[picked].set(jnp.exp(log_sharp))
    below = jnp.clip(jax.random.normal(second_key, (COMPONENTS, D, D)), -6.0, 6.0) * (spread / math.sqrt(D))
    lower_mask = jnp.tril(jnp.ones((D, D), jnp.float32), -1)
    values = below * lower_mask[None] + diagonal[:, :, None] * jnp.eye(D, dtype=jnp.float32)[None]
    return values.astype(jnp.float32).astype(jnp.bfloat16)


def level_of(stream_key, shape, cuts, least, high):
    factor_of, own = 1.0, jax.random.fold_in(stream_key, 6)
    for position, blocks in cuts:
        draws = jnp.exp(jax.random.uniform(jax.random.fold_in(own, position), (blocks,), jnp.float32, least / len(cuts), high / len(cuts)))
        factor_of = factor_of * jnp.repeat(draws, shape[position] // blocks).reshape([-1 if axis == position else 1 for axis in range(len(shape))])
    return factor_of


def setup_inputs(seed: int = 0) -> dict:
    seeds = jax.random.split(jax.random.key(seed), 5)
    return {
        "vectors": draw_vectors(jax.random.fold_in(seeds[4], 71), 0),
        "centers": draw_centers(jax.random.fold_in(seeds[4], 71), 0),
        "factors": draw_factors(jax.random.fold_in(seeds[4], 71), 0),
        "mixing": jnp.clip(jnp.exp(math.log(0.005859375) - 2.3025851 * jax.random.uniform(seeds[3], (COMPONENTS,), jnp.float32) ** level_of(seeds[3], (COMPONENTS,), ((0, 32),), -0.2, 0.2)), 0.0005859375, 0.005859375),
    }


anneal = 1.0
step_weight = 0.5
ridge_term = 0.01
normal_offset = 0.9189385332046727
exact_mode = lax.Precision.HIGHEST

def reference(vectors, centers, factors, mixing):
    vector_total, features = vectors.shape
    wide_vectors = vectors.astype(jnp.float32)
    identity = jnp.eye(features, dtype=jnp.float32)

    def density(component):
        factor, center = component
        factor_wide = factor.astype(jnp.float32)
        whitened = jnp.dot(vectors.astype(jnp.float32), factor.T.astype(jnp.float32), preferred_element_type=jnp.float32) - jnp.dot(factor_wide, center, precision=exact_mode)[None, :]
        return jnp.sum(jnp.log(jnp.diagonal(factor_wide))) - 0.5 * jnp.sum(whitened * whitened, axis=1)
    log_density = lax.map(density, (factors, centers))
    scores = anneal * (log_density + jnp.log(mixing)[:, None] - features * normal_offset)
    row_max = jnp.max(scores, axis=0)
    exponent = jnp.exp(scores - row_max[None, :])
    col_total = jnp.sum(exponent, axis=0)
    shares = exponent / col_total[None, :]
    evidence = (row_max + jnp.log(col_total)) / anneal

    def update(component):
        factor, center, prior_weight, share_row = component
        counts = jnp.sum(share_row)
        first_moment = jnp.dot(share_row, wide_vectors, precision=exact_mode)
        weighted = share_row[:, None] * wide_vectors
        gram_matrix = jnp.dot(weighted.T, wide_vectors, precision=exact_mode)
        kept_share = (1.0 - step_weight) * prior_weight
        weight = kept_share + step_weight * counts / vector_total
        mean_vector = (kept_share * center + step_weight * first_moment / vector_total) / weight
        moment_part = (kept_share * jnp.outer(center, center) + step_weight * gram_matrix / vector_total) / weight - jnp.outer(mean_vector, mean_vector)
        inverse = lax.linalg.triangular_solve(factor.astype(jnp.float32), identity, left_side=True, lower=True)
        covariance = kept_share / weight * jnp.dot(inverse, inverse.T, precision=exact_mode) + moment_part + ridge_term * identity
        cholesky_factor = jnp.linalg.cholesky(covariance)
        refreshed = lax.linalg.triangular_solve(cholesky_factor, identity, left_side=True, lower=True)
        return (refreshed, mean_vector, weight)
    new_factors, new_means, new_weights = lax.map(update, (factors, centers, mixing, shares))
    return (new_factors, new_means, new_weights, evidence)
```

```python
import jax
import jax.numpy as jnp
from jax import lax
from jax.experimental import pallas as pl
from jax.experimental.pallas import tpu as pltpu
from jax.sharding import PartitionSpec as P

step_weight = 0.5
ridge_term = 0.01
normal_offset = 0.9189385332046727
exact_mode = lax.Precision.HIGHEST
PANEL = 32
SUB = 16
f32 = jnp.float32
bf16 = jnp.bfloat16


def in_vmem(count):
    return [pl.BlockSpec(memory_space=pltpu.VMEM)] * count


def call(body, out_shape, scalars, *args, scratch=(), flops=0):
    single = not isinstance(out_shape, (list, tuple))
    return pl.pallas_call(
        body,
        out_shape=out_shape,
        in_specs=[pl.BlockSpec(memory_space=pltpu.SMEM)] + in_vmem(len(args)),
        out_specs=in_vmem(1)[0] if single else in_vmem(len(out_shape)),
        scratch_shapes=list(scratch),
        cost_estimate=pl.CostEstimate(flops=flops, transcendentals=0, bytes_accessed=0),
    )(scalars, *args)


def shape(dims, dtype=f32):
    return jax.ShapeDtypeStruct(dims, dtype)


def eye_of(size):
    rows = lax.broadcasted_iota(jnp.int32, (size, size), 0)
    cols = lax.broadcasted_iota(jnp.int32, (size, size), 1)
    return rows, cols


def three_parts(wide):
    high = wide.astype(bf16)
    rest = wide - high.astype(f32)
    mid = rest.astype(bf16)
    low = (rest - mid.astype(f32)).astype(bf16)
    return high, mid, low


def spread_body(where_ref, vectors_ref, factors_ref, out_ref):
    half = vectors_ref[:, pl.ds(pl.multiple_of(where_ref[1] * 128, 128), 128)]
    for peer in range(out_ref.shape[0]):
        out_ref[peer, :128, :] = half
        out_ref[peer, 128:144, :] = factors_ref[peer, :, :128]
        out_ref[peer, 144:160, :] = factors_ref[peer, :, 128:]


def gather_factor(got_ref, factor_ref):
    for peer in range(16):
        factor_ref[16 * peer : 16 * peer + 16, :128] = got_ref[peer, 128:144, :]
        factor_ref[16 * peer : 16 * peer + 16, 128:] = got_ref[peer, 144:160, :]


def score_body(where_ref, got_ref, other_ref, centers_ref, mixing_ref, out_ref, factor_ref):
    position, core = where_ref[0], where_ref[1]
    gather_factor(got_ref, factor_ref)
    wide = factor_ref[...].astype(f32)
    center = centers_ref[pl.ds(position, 1), :]
    shifted = jnp.sum(wide * center, axis=1, keepdims=True)
    rows, cols = eye_of(256)
    diagonal = jnp.sum(jnp.where(rows == cols, wide, 0.0), axis=1, keepdims=True)
    log_diag = jnp.sum(jnp.log(diagonal), axis=0, keepdims=True)
    log_mix = jnp.log(mixing_ref[pl.ds(position, 1), :])
    mine = factor_ref[:, pl.ds(pl.multiple_of(core * 128, 128), 128)]
    rest = factor_ref[:, pl.ds(pl.multiple_of((1 - core) * 128, 128), 128)]
    over_lanes = (((1,), (1,)), ((), ()))
    for pair in range(8):
        ours = got_ref[2 * pair : 2 * pair + 2, :128, :].reshape(256, 128)
        theirs = other_ref[2 * pair : 2 * pair + 2, :128, :].reshape(256, 128)
        whitened = lax.dot_general(mine, ours, over_lanes, preferred_element_type=f32)
        whitened += lax.dot_general(rest, theirs, over_lanes, preferred_element_type=f32)
        whitened -= shifted
        density = log_diag - 0.5 * jnp.sum(whitened * whitened, axis=0, keepdims=True)
        scores = density + log_mix[:, :1] - 256 * normal_offset
        out_ref[2 * pair] = scores[:, :128]
        out_ref[2 * pair + 1] = scores[:, 128:]


def invert_body(where_ref, got_ref, out_ref, factor_ref, inverse_ref):
    gather_factor(got_ref, factor_ref)
    rows, cols = eye_of(256)
    factor = factor_ref[...]
    diagonal = jnp.sum(jnp.where(rows == cols, factor.astype(f32), 0.0), axis=1, keepdims=True)
    inverse_ref[...] = jnp.where(rows == cols, 1.0 / diagonal, 0.0)

    def double(level, unused):
        inverse = inverse_ref[...]
        below = (rows >> (level + 1) == cols >> (level + 1)) & (rows >> level > cols >> level)
        step = jnp.where(below, factor_ref[...].astype(f32), 0.0)
        moved = jnp.dot(inverse, step, precision=exact_mode, preferred_element_type=f32)
        inverse_ref[...] = inverse - jnp.dot(
            moved, inverse, precision=exact_mode, preferred_element_type=f32
        )
        return unused

    lax.fori_loop(0, 8, double, 0)
    inverse = inverse_ref[...]
    out_ref[...] = lax.dot_general(
        inverse, inverse, (((1,), (1,)), ((), ())), precision=exact_mode, preferred_element_type=f32
    )


def order_body(where_ref, got_ref, other_ref, plain_ref, turned_ref):
    core = where_ref[1]
    ours = pl.ds(pl.multiple_of(core * 128, 128), 128)
    theirs = pl.ds(pl.multiple_of((1 - core) * 128, 128), 128)
    for block in range(16):
        mine, rest = got_ref[block, :128, :], other_ref[block, :128, :]
        plain_ref[128 * block : 128 * block + 128, ours] = mine
        plain_ref[128 * block : 128 * block + 128, theirs] = rest
        turned_ref[block, ours, :] = mine.astype(f32).T.astype(bf16)
        turned_ref[block, theirs, :] = rest.astype(f32).T.astype(bf16)


def partial_body(where_ref, scores_ref, out_ref):
    scores = scores_ref[:, 0, :]
    top = jnp.max(scores, axis=0, keepdims=True)
    total = jnp.sum(jnp.exp(scores - top), axis=0, keepdims=True)
    both = jnp.concatenate([top, total], axis=0)
    for peer in range(out_ref.shape[0]):
        out_ref[peer] = both


def share_body(where_ref, scores_ref, pairs_ref, shares_ref, evidence_ref):
    tops, totals = pairs_ref[:, 0, :], pairs_ref[:, 1, :]
    top = jnp.max(tops, axis=0, keepdims=True)
    total = jnp.sum(totals * jnp.exp(tops - top), axis=0, keepdims=True)
    evidence_ref[...] = top + jnp.log(total)
    shares = jnp.exp(scores_ref[:, 0, :] - top) / total
    for peer in range(shares_ref.shape[0]):
        shares_ref[peer] = shares


def eliminate(left_ref, right_ref, out_ref):
    size, panel, sub = 256, PANEL, SUB
    tiles = panel // 8
    in_tile = lax.broadcasted_iota(jnp.int32, (8, 128), 0)
    for start in range(0, size, panel):
        stop = start + panel
        first = start // 128
        left_tiles = list(range(first, 2))
        right_tiles = list(range(0, (stop - 1) // 128 + 1))
        rows = [
            [left_ref[start + 8 * i : start + 8 * i + 8, 128 * t : 128 * t + 128] for i in range(tiles)]
            for t in left_tiles
        ] + [
            [right_ref[start + 8 * i : start + 8 * i + 8, 128 * t : 128 * t + 128] for i in range(tiles)]
            for t in right_tiles
        ]
        scale = [jnp.zeros((8, 128), f32) for i in range(tiles)]
        for begin in range(0, panel, sub):
            lane = start % 128 + begin
            columns = [
                {
                    i: jnp.broadcast_to(rows[0][i][:, lane + k : lane + k + 1], (8, 128))
                    for i in range((begin + k) // 8, tiles)
                }
                for k in range(sub)
            ]
            for k in range(sub):
                row = begin + k
                tile, place = row // 8, row % 8
                column = columns[k]
                pivot = jnp.broadcast_to(column[tile][place : place + 1, :], (8, 128))
                root = lax.rsqrt(pivot)
                weight = root * root
                ratio = {i: column[i] * weight for i in range(tile, tiles)}
                ratio[tile] = jnp.where(in_tile > place, ratio[tile], 0.0)
                scale[tile] = jnp.where(in_tile == place, root, scale[tile])
                for later in range(k + 1, sub):
                    other = begin + later
                    factor = jnp.broadcast_to(
                        column[other // 8][other % 8 : other % 8 + 1, :], (8, 128)
                    )
                    for i in range(other // 8, tiles):
                        columns[later][i] = columns[later][i] - ratio[i] * factor
                for group in rows:
                    base = jnp.broadcast_to(group[tile][place : place + 1, :], (8, 128))
                    for i in range(tile, tiles):
                        group[i] = group[i] - ratio[i] * base
        solved = [
            jnp.concatenate([group[i] * scale[i] for i in range(tiles)], axis=0) for group in rows
        ]
        left = solved[: len(left_tiles)]
        right = solved[len(left_tiles) :]
        for piece in range(panel // 16):
            block = start // 16 + piece
            for t in range(2):
                lanes = slice(128 * t, 128 * t + 128)
                if t in right_tiles:
                    out_ref[block, :, lanes] = right[t][16 * piece : 16 * piece + 16, :]
                else:
                    out_ref[block, :, lanes] = jnp.zeros((16, 128), f32)
        if stop == size:
            break
        if stop % 128 == 0:
            left, left_tiles = left[1:], left_tiles[1:]
        wide = jnp.concatenate(left, axis=1)
        high, mid, low = three_parts(wide)
        turned = jnp.concatenate([high, high, mid, high, low, mid], axis=0)
        whole = jnp.concatenate(left + right, axis=1)
        high, mid, low = three_parts(whole)
        straight = jnp.concatenate([high, mid, high, low, high, mid], axis=0)
        change = lax.dot_general(
            turned, straight, (((0,), (0,)), ((), ())), preferred_element_type=f32
        )
        skip = stop - 128 * left_tiles[0]
        for position, t in enumerate(left_tiles):
            lanes = slice(128 * t, 128 * t + 128)
            left_ref[stop:, lanes] -= change[skip:, 128 * position : 128 * position + 128]
        for position, t in enumerate(right_tiles):
            lanes = slice(128 * t, 128 * t + 128)
            position += len(left_tiles)
            right_ref[stop:, lanes] -= change[skip:, 128 * position : 128 * position + 128]


def refactor_body(
    where_ref, shares_ref, plain_ref, turned_ref, square_ref, centers_ref, mixing_ref,
    out_ref, left_ref, right_ref,
):
    position = where_ref[0]
    vector_total = plain_ref.shape[0]
    share = shares_ref[:, pl.ds(position, 1), :].reshape(16, 128)
    gram = jnp.zeros((256, 256), f32)
    moment = jnp.zeros((256, 128), f32)
    for pair in range(8):
        weighted = []
        for block in (2 * pair, 2 * pair + 1):
            weighted.append(turned_ref[block].astype(f32) * share[block : block + 1, :])
            moment += weighted[-1]
        vectors = plain_ref[256 * pair : 256 * pair + 256, :]
        for part in three_parts(jnp.concatenate(weighted, axis=1)):
            gram += jnp.dot(part, vectors, preferred_element_type=f32)
    counts = jnp.sum(jnp.sum(share, axis=1, keepdims=True), axis=0, keepdims=True)
    moment = jnp.sum(moment, axis=1, keepdims=True)
    rows, cols = eye_of(256)
    same = rows == cols
    prior = mixing_ref[pl.ds(position, 1), :][:, :1]
    kept = (1.0 - step_weight) * prior
    weight = kept + step_weight * counts / vector_total
    center = centers_ref[pl.ds(position, 1), :]
    center_down = jnp.sum(jnp.where(same, center, 0.0), axis=1, keepdims=True)
    mean_down = (kept * center_down + step_weight * moment / vector_total) / weight
    mean = jnp.sum(jnp.where(same, mean_down, 0.0), axis=0, keepdims=True)
    left_ref[...] = (
        (kept / weight) * square_ref[...]
        + ((kept * center_down) * center + (step_weight / vector_total) * gram) / weight
        - mean_down * mean
        + jnp.where(same, ridge_term, 0.0)
    )
    right_ref[...] = jnp.where(same, 1.0, 0.0)
    eliminate(left_ref, right_ref, out_ref)


def means_body(where_ref, shares_ref, plain_ref, centers_ref, mixing_ref, means_ref, weights_ref):
    vector_total = plain_ref.shape[0]
    moment = jnp.zeros((16, 256), f32)
    counts = jnp.zeros((16, 128), f32)
    for block in range(16):
        share = shares_ref[block]
        counts += share
        vectors = plain_ref[128 * block : 128 * block + 128, :]
        for part in three_parts(share):
            moment += jnp.dot(part, vectors, preferred_element_type=f32)
    counts = jnp.sum(counts, axis=1, keepdims=True)
    kept = (1.0 - step_weight) * mixing_ref[...]
    weights = kept + step_weight * counts / vector_total
    weights_ref[...] = weights
    means_ref[...] = (
        kept[:, :1] * centers_ref[...] + step_weight * moment / vector_total
    ) / weights[:, :1]


def exchanged(array, axis):
    return lax.all_to_all(array, axis, split_axis=0, concat_axis=0, tiled=True)


def local(vectors, centers, factors, mixing):
    groups, peers = lax.axis_size("dp"), lax.axis_size("comp")
    where = jnp.stack([lax.axis_index("dp"), lax.axis_index("comp") % 2]).astype(jnp.int32)
    mixing_wide = jnp.broadcast_to(mixing[:, None], (16, 128))
    spread = call(spread_body, shape((groups, 160, 128), bf16), where, vectors, factors)
    got = exchanged(spread, "dp")
    other = lax.ppermute(got, "comp", [(i, i ^ 1) for i in range(peers)])
    scores = call(
        score_body, shape((16, 1, 128)), where, got, other, centers, mixing_wide,
        scratch=[pltpu.VMEM((256, 256), bf16)], flops=1 << 29,
    )
    scores_here = exchanged(scores, "dp")
    square = call(
        invert_body, shape((256, 256)), where, got,
        scratch=[pltpu.VMEM((256, 256), bf16), pltpu.VMEM((256, 256), f32)], flops=1 << 32,
    )
    plain, turned = call(
        order_body, [shape((2048, 256), bf16), shape((16, 256, 128), bf16)], where, got, other,
        flops=1 << 30,
    )
    partial = call(partial_body, shape((peers, 2, 128)), where, scores_here)
    pairs = exchanged(partial, "comp")
    shares, evidence = call(
        share_body, [shape((groups, 16, 128)), shape((1, 128))], where, scores_here, pairs
    )
    shares_all = exchanged(shares, "dp")
    refreshed = call(
        refactor_body, shape((16, 16, 256)), where, shares_all, plain, turned, square, centers,
        mixing_wide, scratch=[pltpu.VMEM((256, 256), f32)] * 2, flops=1 << 32,
    )
    new_factors = exchanged(refreshed, "dp")
    new_means, new_weights = call(
        means_body, [shape((16, 256)), shape((16, 128))], where, shares_all, plain, centers,
        mixing_wide, flops=1 << 28,
    )
    return new_factors, new_means, new_weights[:, 0], evidence.reshape(128)


def solution(mesh):
    return jax.shard_map(
        local,
        mesh=mesh,
        in_specs=(P("dp", None), P("comp", None), P("comp", "dp", None), P("comp")),
        out_specs=(P("comp", "dp", None), P("comp", None), P("comp"), P("dp")),
        check_vma=False,
    )
```

```python
import jax
import jax.numpy as jnp
from jax import lax
from jax.experimental import pallas as pl
from jax.experimental.pallas import tpu as pltpu
from jax.sharding import PartitionSpec as P

step_weight = 0.5
ridge_term = 0.01
normal_offset = 0.9189385332046727
exact_mode = lax.Precision.HIGHEST
PANEL = 32
SUB = 16
f32 = jnp.float32
bf16 = jnp.bfloat16


def call(body, out_shape, *args, scratch=(), flops=0):
    single = not isinstance(out_shape, (list, tuple))
    vmem = pl.BlockSpec(memory_space=pltpu.VMEM)
    args = [pltpu.with_memory_space_constraint(arg, pltpu.VMEM) for arg in args]
    return pl.pallas_call(
        body,
        out_shape=out_shape,
        in_specs=[vmem] * len(args),
        out_specs=vmem if single else [vmem] * len(out_shape),
        scratch_shapes=list(scratch),
        cost_estimate=pl.CostEstimate(flops=flops, transcendentals=0, bytes_accessed=0),
        compiler_params=pltpu.CompilerParams(vmem_limit_bytes=12 << 20),
    )(*args)


def place():
    return lax.axis_index("dp"), lax.axis_index("comp") % 2


def shape(dims, dtype=f32):
    return pltpu.VMEM(dims, dtype)


def far(dims, dtype=f32):
    return jax.ShapeDtypeStruct(dims, dtype)


def own_of(row_ref, position):
    row = row_ref[...]
    lanes = lax.broadcasted_iota(jnp.int32, row.shape, 1)
    return jnp.sum(jnp.where(lanes == position, row, 0.0), axis=1, keepdims=True)


def eye_of(size):
    rows = lax.broadcasted_iota(jnp.int32, (size, size), 0)
    cols = lax.broadcasted_iota(jnp.int32, (size, size), 1)
    return rows, cols


def three_parts(wide):
    high = wide.astype(bf16)
    rest = wide - high.astype(f32)
    mid = rest.astype(bf16)
    low = (rest - mid.astype(f32)).astype(bf16)
    return high, mid, low


def spread_body(vectors_ref, factors_ref, out_ref):
    unused, core = place()
    half = vectors_ref[:, pl.ds(pl.multiple_of(core * 128, 128), 128)]
    for peer in range(out_ref.shape[0]):
        out_ref[peer, :128, :] = half
        out_ref[peer, 128:144, :] = factors_ref[peer, :, :128]
        out_ref[peer, 144:160, :] = factors_ref[peer, :, 128:]


def gather_factor(got_ref, factor_ref):
    for peer in range(16):
        factor_ref[16 * peer : 16 * peer + 16, :128] = got_ref[peer, 128:144, :]
        factor_ref[16 * peer : 16 * peer + 16, 128:] = got_ref[peer, 144:160, :]


def score_body(got_ref, other_ref, centers_ref, mixing_ref, out_ref, factor_ref):
    position, core = place()
    gather_factor(got_ref, factor_ref)
    wide = factor_ref[...].astype(f32)
    center = centers_ref[pl.ds(position, 1), :]
    shifted = jnp.sum(wide * center, axis=1, keepdims=True)
    rows, cols = eye_of(256)
    diagonal = jnp.sum(jnp.where(rows == cols, wide, 0.0), axis=1, keepdims=True)
    log_diag = jnp.sum(jnp.log(diagonal), axis=0, keepdims=True)
    log_mix = jnp.log(own_of(mixing_ref, position))
    mine = factor_ref[:, pl.ds(pl.multiple_of(core * 128, 128), 128)]
    rest = factor_ref[:, pl.ds(pl.multiple_of((1 - core) * 128, 128), 128)]
    over_lanes = (((1,), (1,)), ((), ()))
    for pair in range(8):
        ours = got_ref[2 * pair : 2 * pair + 2, :128, :].reshape(256, 128)
        theirs = other_ref[2 * pair : 2 * pair + 2, :128, :].reshape(256, 128)
        whitened = lax.dot_general(mine, ours, over_lanes, preferred_element_type=f32)
        whitened += lax.dot_general(rest, theirs, over_lanes, preferred_element_type=f32)
        whitened -= shifted
        density = log_diag - 0.5 * jnp.sum(whitened * whitened, axis=0, keepdims=True)
        scores = density + log_mix - 256 * normal_offset
        out_ref[2 * pair] = scores[:, :128]
        out_ref[2 * pair + 1] = scores[:, 128:]


def apart(left, right, **options):
    return jnp.dot(left, right, precision=exact_mode, preferred_element_type=f32)


def invert_body(got_ref, out_ref, factor_ref, inverse_ref):
    gather_factor(got_ref, factor_ref)
    rows, cols = eye_of(128)
    factors = []
    for start in (0, 128):
        factor = factor_ref[start : start + 128, start : start + 128].astype(f32)
        diagonal = jnp.sum(jnp.where(rows == cols, factor, 0.0), axis=1, keepdims=True)
        factors.append(factor)
        inverse_ref[start // 128] = jnp.where(rows == cols, 1.0 / diagonal, 0.0)
    for level in range(7):
        below = (rows >> (level + 1) == cols >> (level + 1)) & (rows >> level > cols >> level)
        for block in range(2):
            inverse = inverse_ref[block]
            step = jnp.where(below, factors[block], 0.0)
            inverse_ref[block] = inverse - apart(apart(inverse, step), inverse)
    first, last = inverse_ref[0], inverse_ref[1]
    corner = -apart(apart(last, factor_ref[128:, :128].astype(f32)), first)
    bottom = jnp.concatenate([corner, last], axis=1)
    whole = jnp.concatenate(
        [jnp.concatenate([first, jnp.zeros((128, 128), f32)], axis=1), bottom], axis=0
    )
    out_ref[...] = lax.dot_general(
        whole, whole, (((1,), (1,)), ((), ())), precision=exact_mode, preferred_element_type=f32
    )


INV_SCRATCH = [pltpu.VMEM((256, 256), bf16), pltpu.VMEM((2, 128, 128), f32)]


def order_body(got_ref, other_ref, plain_ref, turned_ref):
    unused, core = place()
    ours = pl.ds(pl.multiple_of(core * 128, 128), 128)
    theirs = pl.ds(pl.multiple_of((1 - core) * 128, 128), 128)
    for block in range(16):
        mine, rest = got_ref[block, :128, :], other_ref[block, :128, :]
        plain_ref[128 * block : 128 * block + 128, ours] = mine
        plain_ref[128 * block : 128 * block + 128, theirs] = rest
        turned_ref[block, ours, :] = mine.astype(f32).T.astype(bf16)
        turned_ref[block, theirs, :] = rest.astype(f32).T.astype(bf16)


def prepare_body(got_ref, other_ref, square_ref, plain_ref, turned_ref, factor_ref, inverse_ref):
    invert_body(got_ref, square_ref, factor_ref, inverse_ref)
    order_body(got_ref, other_ref, plain_ref, turned_ref)


def partial_body(scores_ref, out_ref):
    scores = scores_ref[:, 0, :]
    top = jnp.max(scores, axis=0, keepdims=True)
    total = jnp.sum(jnp.exp(scores - top), axis=0, keepdims=True)
    both = jnp.concatenate([top, total], axis=0)
    for peer in range(out_ref.shape[0]):
        out_ref[peer] = both


def share_body(scores_ref, pairs_ref, shares_ref, evidence_ref):
    tops, totals = pairs_ref[:, 0, :], pairs_ref[:, 1, :]
    top = jnp.max(tops, axis=0, keepdims=True)
    total = jnp.sum(totals * jnp.exp(tops - top), axis=0, keepdims=True)
    evidence_ref[...] = top + jnp.log(total)
    shares = jnp.exp(scores_ref[:, 0, :] - top) / total
    for peer in range(shares_ref.shape[0]):
        shares_ref[peer] = shares


def eliminate(left_ref, right_ref, out_ref):
    size, panel, sub = 256, PANEL, SUB
    tiles = panel // 8
    in_tile = lax.broadcasted_iota(jnp.int32, (8, 128), 0)
    for start in range(0, size, panel):
        stop = start + panel
        first = start // 128
        left_tiles = list(range(first, 2))
        right_tiles = list(range(0, (stop - 1) // 128 + 1))
        rows = [
            [left_ref[start + 8 * i : start + 8 * i + 8, 128 * t : 128 * t + 128] for i in range(tiles)]
            for t in left_tiles
        ] + [
            [right_ref[start + 8 * i : start + 8 * i + 8, 128 * t : 128 * t + 128] for i in range(tiles)]
            for t in right_tiles
        ]
        scale = [jnp.zeros((8, 128), f32) for i in range(tiles)]
        for begin in range(0, panel, sub):
            lane = start % 128 + begin
            columns = [
                {
                    i: jnp.broadcast_to(rows[0][i][:, lane + k : lane + k + 1], (8, 128))
                    for i in range((begin + k) // 8, tiles)
                }
                for k in range(sub)
            ]
            for k in range(sub):
                row = begin + k
                tile, place = row // 8, row % 8
                column = columns[k]
                pivot = jnp.broadcast_to(column[tile][place : place + 1, :], (8, 128))
                root = lax.rsqrt(pivot)
                weight = root * root
                ratio = {i: column[i] * weight for i in range(tile, tiles)}
                ratio[tile] = jnp.where(in_tile > place, ratio[tile], 0.0)
                scale[tile] = jnp.where(in_tile == place, root, scale[tile])
                for later in range(k + 1, sub):
                    other = begin + later
                    factor = jnp.broadcast_to(
                        column[other // 8][other % 8 : other % 8 + 1, :], (8, 128)
                    )
                    for i in range(other // 8, tiles):
                        columns[later][i] = columns[later][i] - ratio[i] * factor
                for group in rows:
                    base = jnp.broadcast_to(group[tile][place : place + 1, :], (8, 128))
                    for i in range(tile, tiles):
                        group[i] = group[i] - ratio[i] * base
        solved = [
            jnp.concatenate([group[i] * scale[i] for i in range(tiles)], axis=0) for group in rows
        ]
        left = solved[: len(left_tiles)]
        right = solved[len(left_tiles) :]
        for piece in range(panel // 16):
            block = start // 16 + piece
            for t in range(2):
                lanes = slice(128 * t, 128 * t + 128)
                if t in right_tiles:
                    out_ref[block, :, lanes] = right[t][16 * piece : 16 * piece + 16, :]
                else:
                    out_ref[block, :, lanes] = jnp.zeros((16, 128), f32)
        if stop == size:
            break
        if stop % 128 == 0:
            left, left_tiles = left[1:], left_tiles[1:]
        wide = jnp.concatenate(left, axis=1)
        high, mid, low = three_parts(wide)
        turned = jnp.concatenate([high, high, mid, high, low, mid], axis=0)
        whole = jnp.concatenate(left + right, axis=1)
        high, mid, low = three_parts(whole)
        straight = jnp.concatenate([high, mid, high, low, high, mid], axis=0)
        change = lax.dot_general(
            turned, straight, (((0,), (0,)), ((), ())), preferred_element_type=f32
        )
        skip = stop - 128 * left_tiles[0]
        for position, t in enumerate(left_tiles):
            lanes = slice(128 * t, 128 * t + 128)
            left_ref[stop:, lanes] -= change[skip:, 128 * position : 128 * position + 128]
        for position, t in enumerate(right_tiles):
            lanes = slice(128 * t, 128 * t + 128)
            position += len(left_tiles)
            right_ref[stop:, lanes] -= change[skip:, 128 * position : 128 * position + 128]


def refactor_body(
    shares_ref, plain_ref, turned_ref, square_ref, centers_ref, mixing_ref,
    out_ref, left_ref, right_ref,
):
    position, unused = place()
    vector_total = plain_ref.shape[0]
    share = shares_ref[:, pl.ds(position, 1), :].reshape(16, 128)
    gram = jnp.zeros((256, 256), f32)
    moment = jnp.zeros((256, 128), f32)
    for pair in range(8):
        weighted = []
        for block in (2 * pair, 2 * pair + 1):
            weighted.append(turned_ref[block].astype(f32) * share[block : block + 1, :])
            moment += weighted[-1]
        vectors = plain_ref[256 * pair : 256 * pair + 256, :]
        for part in three_parts(jnp.concatenate(weighted, axis=1)):
            gram += jnp.dot(part, vectors, preferred_element_type=f32)
    counts = jnp.sum(jnp.sum(share, axis=1, keepdims=True), axis=0, keepdims=True)
    moment = jnp.sum(moment, axis=1, keepdims=True)
    rows, cols = eye_of(256)
    same = rows == cols
    prior = own_of(mixing_ref, position)
    kept = (1.0 - step_weight) * prior
    weight = kept + step_weight * counts / vector_total
    center = centers_ref[pl.ds(position, 1), :]
    center_down = jnp.sum(jnp.where(same, center, 0.0), axis=1, keepdims=True)
    mean_down = (kept * center_down + step_weight * moment / vector_total) / weight
    mean = jnp.sum(jnp.where(same, mean_down, 0.0), axis=0, keepdims=True)
    left_ref[...] = (
        (kept / weight) * square_ref[...]
        + ((kept * center_down) * center + (step_weight / vector_total) * gram) / weight
        - mean_down * mean
        + jnp.where(same, ridge_term, 0.0)
    )
    right_ref[...] = jnp.where(same, 1.0, 0.0)
    eliminate(left_ref, right_ref, out_ref)


def means_body(shares_ref, plain_ref, centers_ref, mixing_ref, means_ref, weights_ref):
    vector_total = plain_ref.shape[0]
    moment = jnp.zeros((16, 256), f32)
    counts = jnp.zeros((16, 128), f32)
    for block in range(16):
        share = shares_ref[block]
        counts += share
        vectors = plain_ref[128 * block : 128 * block + 128, :]
        for part in three_parts(share):
            moment += jnp.dot(part, vectors, preferred_element_type=f32)
    counts = jnp.sum(counts, axis=1, keepdims=True)
    rows, cols = eye_of(16)
    prior = jnp.sum(jnp.where(rows == cols, mixing_ref[...], 0.0), axis=1, keepdims=True)
    kept = (1.0 - step_weight) * prior
    weights = kept + step_weight * counts / vector_total
    weights_ref[...] = jnp.sum(jnp.where(rows == cols, weights, 0.0), axis=0, keepdims=True)
    means_ref[...] = (
        kept * centers_ref[...] + step_weight * moment / vector_total
    ) / weights


def exchanged(array, axis):
    return lax.all_to_all(array, axis, split_axis=0, concat_axis=0, tiled=True)


def local(vectors, centers, factors, mixing):
    groups, peers = lax.axis_size("dp"), lax.axis_size("comp")
    priors = mixing.reshape(1, 16)
    spread = call(spread_body, shape((groups, 160, 128), bf16), vectors, factors)
    got = exchanged(spread, "dp")
    other = lax.ppermute(got, "comp", [(i, i ^ 1) for i in range(peers)])
    scores = call(
        score_body, shape((16, 1, 128)), got, other, centers, priors,
        scratch=[pltpu.VMEM((256, 256), bf16)], flops=1 << 29,
    )
    scores, after, after_other = lax.optimization_barrier((scores, got, other))
    scores_here = exchanged(scores, "dp")
    square, plain, turned = call(
        prepare_body,
        [shape((256, 256)), shape((2048, 256), bf16), shape((16, 256, 128), bf16)],
        after, after_other, scratch=INV_SCRATCH, flops=1 << 30,
    )
    scores_here, square, plain, turned = lax.optimization_barrier(
        (scores_here, square, plain, turned)
    )
    partial = call(partial_body, shape((peers, 2, 128)), scores_here)
    pairs = exchanged(partial, "comp")
    shares, evidence = call(
        share_body, [shape((groups, 16, 128)), far((1, 128))], scores_here, pairs
    )
    shares_all = exchanged(shares, "dp")
    refreshed = call(
        refactor_body, shape((16, 16, 256)), shares_all, plain, turned, square, centers,
        priors, scratch=[pltpu.VMEM((256, 256), f32)] * 2, flops=1 << 32,
    )
    new_factors = exchanged(refreshed, "dp")
    new_means, new_weights = call(
        means_body, [far((16, 256)), far((1, 16))], shares_all, plain, centers, priors,
        flops=1 << 28,
    )
    return new_factors, new_means, new_weights.reshape(16), evidence.reshape(128)


def solution(mesh):
    return jax.shard_map(
        local,
        mesh=mesh,
        in_specs=(P("dp", None), P("comp", None), P("comp", "dp", None), P("comp")),
        out_specs=(P("comp", "dp", None), P("comp", None), P("comp"), P("dp")),
        check_vma=False,
    )
```

```python
import jax
import jax.numpy as jnp
from jax import lax
from jax.experimental import pallas as pl
from jax.experimental.pallas import tpu as pltpu
from jax.sharding import PartitionSpec as P

step_weight = 0.5
ridge_term = 0.01
normal_offset = 0.9189385332046727
exact_mode = lax.Precision.HIGHEST
PANEL = 32
SUB = 16
SQUARE, BOTH, START, TABLES = 0, 2, 4, 6
f32 = jnp.float32
bf16 = jnp.bfloat16


def call(body, out_shape, *args, scratch=(), flops=0, near=True):
    single = not isinstance(out_shape, (list, tuple))
    vmem = pl.BlockSpec(memory_space=pltpu.VMEM)
    space = pltpu.VMEM if near else pltpu.HBM
    args = [pltpu.with_memory_space_constraint(arg, space) for arg in args]
    return pl.pallas_call(
        body,
        out_shape=out_shape,
        in_specs=[vmem] * len(args),
        out_specs=vmem if single else [vmem] * len(out_shape),
        scratch_shapes=list(scratch),
        cost_estimate=pl.CostEstimate(flops=flops, transcendentals=0, bytes_accessed=0),
        compiler_params=pltpu.CompilerParams(vmem_limit_bytes=12 << 20),
    )(*args)


def place():
    return lax.axis_index("dp"), lax.axis_index("comp") % 2


def shape(dims, dtype=f32):
    return pltpu.VMEM(dims, dtype)


def far(dims, dtype=f32):
    return jax.ShapeDtypeStruct(dims, dtype)


def own_of(row_ref, position):
    row = row_ref[...]
    lanes = lax.broadcasted_iota(jnp.int32, row.shape, 1)
    return jnp.sum(jnp.where(lanes == position, row, 0.0), axis=1, keepdims=True)


def eye_of(size):
    rows = lax.broadcasted_iota(jnp.int32, (size, size), 0)
    cols = lax.broadcasted_iota(jnp.int32, (size, size), 1)
    return rows, cols


def three_parts(wide):
    high = wide.astype(bf16)
    rest = wide - high.astype(f32)
    mid = rest.astype(bf16)
    low = (rest - mid.astype(f32)).astype(bf16)
    return high, mid, low


def over_lanes(left, right):
    return lax.dot_general(left, right, (((1,), (1,)), ((), ())), preferred_element_type=f32)


def spread_body(vectors_ref, factors_ref, out_ref):
    unused, core = place()
    half = vectors_ref[:, pl.ds(pl.multiple_of(core * 128, 128), 128)]
    for peer in range(out_ref.shape[0]):
        out_ref[peer, :128, :] = half
        out_ref[peer, 128:144, :] = factors_ref[peer, :, :128]
        out_ref[peer, 144:160, :] = factors_ref[peer, :, 128:]


def gather_factor(got_ref, factor_ref):
    for peer in range(16):
        factor_ref[16 * peer : 16 * peer + 16, :128] = got_ref[peer, 128:144, :]
        factor_ref[16 * peer : 16 * peer + 16, 128:] = got_ref[peer, 144:160, :]


def score_body(got_ref, other_ref, centers_ref, mixing_ref, out_ref, factor_ref):
    position, core = place()
    gather_factor(got_ref, factor_ref)
    wide = factor_ref[...].astype(f32)
    center = centers_ref[pl.ds(position, 1), :]
    shifted = jnp.sum(wide * center, axis=1, keepdims=True)
    rows, cols = eye_of(256)
    diagonal = jnp.sum(jnp.where(rows == cols, wide, 0.0), axis=1, keepdims=True)
    log_diag = jnp.sum(jnp.log(diagonal), axis=0, keepdims=True)
    log_mix = jnp.log(own_of(mixing_ref, position))
    mine = factor_ref[:, pl.ds(pl.multiple_of(core * 128, 128), 128)]
    rest = factor_ref[:, pl.ds(pl.multiple_of((1 - core) * 128, 128), 128)]
    for pair in range(8):
        ours = got_ref[2 * pair : 2 * pair + 2, :128, :].reshape(256, 128)
        theirs = other_ref[2 * pair : 2 * pair + 2, :128, :].reshape(256, 128)
        whitened = over_lanes(mine, ours) + over_lanes(rest, theirs)
        whitened -= shifted
        density = log_diag - 0.5 * jnp.sum(whitened * whitened, axis=0, keepdims=True)
        scores = density + log_mix - 256 * normal_offset
        out_ref[2 * pair] = scores[:, :128]
        out_ref[2 * pair + 1] = scores[:, 128:]


def apart(left, right, **options):
    return jnp.dot(left, right, precision=exact_mode, preferred_element_type=f32)


def invert_body(got_ref, tables_ref, factor_ref, inverse_ref):
    gather_factor(got_ref, factor_ref)
    rows, cols = eye_of(128)
    factors = []
    for start in (0, 128):
        factor = factor_ref[start : start + 128, start : start + 128].astype(f32)
        diagonal = jnp.sum(jnp.where(rows == cols, factor, 0.0), axis=1, keepdims=True)
        factors.append(factor)
        inverse_ref[start // 128] = jnp.where(rows == cols, 1.0 / diagonal, 0.0)
    for level in range(7):
        below = (rows >> (level + 1) == cols >> (level + 1)) & (rows >> level > cols >> level)
        for block in range(2):
            inverse = inverse_ref[block]
            step = jnp.where(below, factors[block], 0.0)
            inverse_ref[block] = inverse - apart(apart(inverse, step), inverse)
    first, last = inverse_ref[0], inverse_ref[1]
    corner = -apart(apart(last, factor_ref[128:, :128].astype(f32)), first)
    bottom = jnp.concatenate([corner, last], axis=1)
    whole = jnp.concatenate(
        [jnp.concatenate([first, jnp.zeros((128, 128), f32)], axis=1), bottom], axis=0
    )
    square = lax.dot_general(
        whole, whole, (((1,), (1,)), ((), ())), precision=exact_mode, preferred_element_type=f32
    )
    rows, cols = eye_of(256)
    diagonal = jnp.where(rows == cols, square, 0.0)
    down = lax.rsqrt(1.0 + jnp.sum(diagonal, axis=1, keepdims=True))
    across = lax.rsqrt(1.0 + jnp.sum(diagonal, axis=0, keepdims=True))
    both = down * across
    tables = (square * both, both, jnp.where(rows == cols, across, 0.0))
    for place, table in zip((SQUARE, BOTH, START), tables):
        tables_ref[place] = table[:, :128]
        tables_ref[place + 1] = table[:, 128:]


INV_SCRATCH = [pltpu.VMEM((256, 256), bf16), pltpu.VMEM((2, 128, 128), f32)]


def order_body(got_ref, other_ref, turned_ref):
    unused, core = place()
    ours = pl.ds(pl.multiple_of(core * 128, 128), 128)
    theirs = pl.ds(pl.multiple_of((1 - core) * 128, 128), 128)
    for block in range(16):
        turned_ref[block, ours, :] = got_ref[block, :128, :].T
        turned_ref[block, theirs, :] = other_ref[block, :128, :].T


def prepare_body(got_ref, other_ref, tables_ref, turned_ref, factor_ref, inverse_ref):
    invert_body(got_ref, tables_ref, factor_ref, inverse_ref)
    order_body(got_ref, other_ref, turned_ref)


def partial_body(scores_ref, out_ref):
    scores = scores_ref[:, 0, :]
    top = jnp.max(scores, axis=0, keepdims=True)
    total = jnp.sum(jnp.exp(scores - top), axis=0, keepdims=True)
    both = jnp.concatenate([top, total], axis=0)
    for peer in range(out_ref.shape[0]):
        out_ref[peer] = both


def share_body(scores_ref, pairs_ref, shares_ref, evidence_ref):
    tops, totals = pairs_ref[:, 0, :], pairs_ref[:, 1, :]
    top = jnp.max(tops, axis=0, keepdims=True)
    total = jnp.sum(totals * jnp.exp(tops - top), axis=0, keepdims=True)
    evidence_ref[...] = top + jnp.log(total)
    shares = jnp.exp(scores_ref[:, 0, :] - top) / total
    for peer in range(shares_ref.shape[0]):
        shares_ref[peer] = shares


def same_row(tile, row):
    return jnp.broadcast_to(tile[row : row + 1, :], tile.shape)


def eliminate(work_ref, tables_ref, out_ref):
    size, panel, sub = 256, PANEL, SUB
    tiles = panel // 8
    in_tile = lax.broadcasted_iota(jnp.int32, (8, 128), 0)
    lane_of = lax.broadcasted_iota(jnp.int32, (8, 128), 1)
    far_lane = lax.broadcasted_iota(jnp.int32, (1, 128), 1)
    for start in range(0, size, panel):
        stop = start + panel
        near = start // 128
        rows = [
            [work_ref[start + 8 * i : start + 8 * i + 8, 128 * t : 128 * t + 128] for i in range(tiles)]
            for t in range(2)
        ]
        scale = [jnp.zeros((8, 128), f32) for i in range(tiles)]
        for begin in range(0, panel, sub):
            lane = start % 128 + begin
            columns = [
                {
                    i: jnp.broadcast_to(rows[near][i][:, lane + k : lane + k + 1], (8, 128))
                    for i in range((begin + k) // 8, tiles)
                }
                for k in range(sub)
            ]
            cleared = (lane_of >= lane) & (lane_of < lane + sub)
            for i in range(tiles):
                fresh = tables_ref[START + near, start + 8 * i : start + 8 * i + 8, :]
                rows[near][i] = jnp.where(cleared, fresh, rows[near][i])
            for k in range(0, sub, 2):
                row = begin + k
                tile, place = row // 8, row % 8
                one, two = columns[k], columns[k + 1]
                a, b = same_row(one[tile], place), same_row(one[tile], place + 1)
                d = same_row(two[tile], place + 1)
                root = lax.rsqrt(a * d - b * b)
                inverse = root * root
                root_a = lax.rsqrt(a)
                raw = {
                    i: (one[i] * d - two[i] * b, two[i] * a - one[i] * b)
                    for i in range(tile, tiles)
                }
                below = in_tile > place + 1
                raw[tile] = tuple(jnp.where(below, part, 0.0) for part in raw[tile])
                ratio = {i: (raw[i][0] * inverse, raw[i][1] * inverse) for i in raw}
                for later in range(k + 2, sub):
                    other = begin + later
                    f = same_row(one[other // 8], other % 8)
                    g = same_row(two[other // 8], other % 8)
                    for i in range(other // 8, tiles):
                        if later < k + 4:
                            change = (raw[i][0] * f + raw[i][1] * g) * inverse
                        else:
                            change = ratio[i][0] * f + ratio[i][1] * g
                        columns[later][i] = columns[later][i] - change
                ratio[tile] = (
                    jnp.where(in_tile == place + 1, b * (root_a * root_a), ratio[tile][0]),
                    ratio[tile][1],
                )
                for group in rows:
                    f, g = same_row(group[tile], place), same_row(group[tile], place + 1)
                    for i in range(tile, tiles):
                        group[i] = group[i] - (ratio[i][0] * f + ratio[i][1] * g)
                scale[tile] = jnp.where(in_tile == place, root_a, scale[tile])
                scale[tile] = jnp.where(in_tile == place + 1, root * (a * root_a), scale[tile])
        solved = [
            jnp.concatenate([group[i] * scale[i] for i in range(tiles)], axis=0) for group in rows
        ]
        for t in range(2):
            lanes = slice(128 * t, 128 * t + 128)
            done = jnp.where(far_lane + 128 * t < stop, solved[t], 0.0)
            for piece in range(panel // 16):
                out_ref[start // 16 + piece, :, lanes] = done[16 * piece : 16 * piece + 16, :]
        if stop == size:
            break
        high, mid, low = three_parts(jnp.concatenate(solved, axis=1))
        straight = jnp.concatenate([high, mid, high, low, high, mid], axis=0)
        turned = jnp.concatenate([high, high, mid, high, low, mid], axis=0)
        inside = (far_lane + 128 * near >= start) & (far_lane + 128 * near < stop)
        for mine in range(stop // 128, 2):
            change = lax.dot_general(
                turned[:, 128 * mine : 128 * mine + 128],
                straight,
                (((0,), (0,)), ((), ())),
                preferred_element_type=f32,
            )
            begin = max(stop, 128 * mine)
            skip = begin - 128 * mine
            for t in range(2):
                lanes = slice(128 * t, 128 * t + 128)
                kept = work_ref[begin : 128 * mine + 128, lanes]
                if t == near:
                    kept = jnp.where(inside, 0.0, kept)
                work_ref[begin : 128 * mine + 128, lanes] = kept - change[skip:, lanes]


def refactor_body(
    shares_ref, turned_ref, tables_ref, centers_ref, mixing_ref, out_ref, work_ref
):
    position, unused = place()
    vector_total = turned_ref.shape[0] * turned_ref.shape[2]
    share = shares_ref[:, pl.ds(position, 1), :].reshape(16, 128)
    gram = jnp.zeros((256, 256), f32)
    moment = jnp.zeros((256, 128), f32)
    for pair in range(8):
        weighted = []
        for block in (2 * pair, 2 * pair + 1):
            weighted.append(turned_ref[block].astype(f32) * share[block : block + 1, :])
            moment += weighted[-1]
        vectors = jnp.concatenate([turned_ref[2 * pair], turned_ref[2 * pair + 1]], axis=1)
        for part in three_parts(jnp.concatenate(weighted, axis=1)):
            gram += over_lanes(part, vectors)
    counts = jnp.sum(jnp.sum(share, axis=1, keepdims=True), axis=0, keepdims=True)
    moment = jnp.sum(moment, axis=1, keepdims=True)
    rows, cols = eye_of(256)
    same = rows == cols
    prior = own_of(mixing_ref, position)
    kept = (1.0 - step_weight) * prior
    weight = kept + step_weight * counts / vector_total
    center = centers_ref[pl.ds(position, 1), :]
    center_down = jnp.sum(jnp.where(same, center, 0.0), axis=1, keepdims=True)
    mean_down = (kept * center_down + step_weight * moment / vector_total) / weight
    mean = jnp.sum(jnp.where(same, mean_down, 0.0), axis=0, keepdims=True)
    moment_part = (
        ((kept * center_down) * center + (step_weight / vector_total) * gram) / weight
        - mean_down * mean
        + jnp.where(same, ridge_term, 0.0)
    )
    for t in range(2):
        lanes = slice(128 * t, 128 * t + 128)
        work_ref[:, lanes] = (kept / weight) * tables_ref[SQUARE + t] + moment_part[:, lanes] * (
            tables_ref[BOTH + t]
        )
    eliminate(work_ref, tables_ref, out_ref)


def means_body(shares_ref, turned_ref, centers_ref, mixing_ref, means_ref, weights_ref):
    vector_total = turned_ref.shape[0] * turned_ref.shape[2]
    moment = jnp.zeros((16, 256), f32)
    counts = jnp.zeros((16, 128), f32)
    for block in range(16):
        share = shares_ref[block]
        counts += share
        for part in three_parts(share):
            moment += over_lanes(part, turned_ref[block])
    counts = jnp.sum(counts, axis=1, keepdims=True)
    rows, cols = eye_of(16)
    prior = jnp.sum(jnp.where(rows == cols, mixing_ref[...], 0.0), axis=1, keepdims=True)
    kept = (1.0 - step_weight) * prior
    weights = kept + step_weight * counts / vector_total
    weights_ref[...] = jnp.sum(jnp.where(rows == cols, weights, 0.0), axis=0, keepdims=True)
    means_ref[...] = (
        kept * centers_ref[...] + step_weight * moment / vector_total
    ) / weights


def exchanged(array, axis):
    return lax.all_to_all(array, axis, split_axis=0, concat_axis=0, tiled=True)


def local(vectors, centers, factors, mixing):
    groups, peers = lax.axis_size("dp"), lax.axis_size("comp")
    priors = mixing.reshape(1, 16)
    spread = call(spread_body, shape((groups, 160, 128), bf16), vectors, factors, near=False)
    got = exchanged(spread, "dp")
    other = lax.ppermute(got, "comp", [(i, i ^ 1) for i in range(peers)])
    scores = call(
        score_body, shape((16, 1, 128)), got, other, centers, priors,
        scratch=[pltpu.VMEM((256, 256), bf16)], flops=1 << 29,
    )
    scores, after, after_other = lax.optimization_barrier((scores, got, other))
    scores_here = exchanged(scores, "dp")
    tables, turned = call(
        prepare_body,
        [shape((TABLES, 256, 128)), shape((16, 256, 128), bf16)],
        after, after_other, scratch=INV_SCRATCH, flops=1 << 30,
    )
    scores_here, tables, turned = lax.optimization_barrier((scores_here, tables, turned))
    partial = call(partial_body, shape((peers, 2, 128)), scores_here)
    pairs = exchanged(partial, "comp")
    shares, evidence = call(
        share_body, [shape((groups, 16, 128)), far((1, 128))], scores_here, pairs
    )
    shares_all = exchanged(shares, "dp")
    refreshed = call(
        refactor_body, shape((16, 16, 256)), shares_all, turned, tables, centers,
        priors, scratch=[pltpu.VMEM((256, 256), f32)], flops=1 << 32,
    )
    new_factors = exchanged(refreshed, "dp")
    new_means, new_weights = call(
        means_body, [far((16, 256)), far((1, 16))], shares_all, turned, centers, priors,
        flops=1 << 28,
    )
    return new_factors, new_means, new_weights.reshape(16), evidence.reshape(128)


def solution(mesh):
    return jax.shard_map(
        local,
        mesh=mesh,
        in_specs=(P("dp", None), P("comp", None), P("comp", "dp", None), P("comp")),
        out_specs=(P("comp", "dp", None), P("comp", None), P("comp"), P("dp")),
        check_vma=False,
    )
```

```python
import jax
import jax.numpy as jnp
from jax import lax
from jax.experimental import pallas as pl
from jax.experimental.pallas import tpu as pltpu
from jax.sharding import PartitionSpec as P

step_weight = 0.5
ridge_term = 0.01
normal_offset = 0.9189385332046727
exact_mode = lax.Precision.HIGHEST
PANEL = 32
SUB = 16
SQUARE, BOTH, START, TABLES = 0, 2, 4, 6
f32 = jnp.float32
bf16 = jnp.bfloat16


def call(body, out_shape, *args, scratch=(), flops=0, near=True):
    single = not isinstance(out_shape, (list, tuple))
    vmem = pl.BlockSpec(memory_space=pltpu.VMEM)
    hbm = pl.BlockSpec(memory_space=pltpu.HBM)
    space = pltpu.VMEM if near else pltpu.HBM
    args = [pltpu.with_memory_space_constraint(arg, space) for arg in args]
    return pl.pallas_call(
        body,
        out_shape=out_shape,
        in_specs=[vmem] * len(args),
        out_specs=vmem if single else [
            hbm if out.memory_space == pltpu.HBM else vmem for out in out_shape
        ],
        scratch_shapes=list(scratch),
        cost_estimate=pl.CostEstimate(flops=flops, transcendentals=0, bytes_accessed=0),
        compiler_params=pltpu.CompilerParams(vmem_limit_bytes=12 << 20),
    )(*args)


def place():
    return lax.axis_index("dp"), lax.axis_index("comp") % 2


def shape(dims, dtype=f32):
    return pltpu.VMEM(dims, dtype)


def far(dims, dtype=f32):
    return pltpu.HBM(dims, dtype)


def own_of(row_ref, position):
    row = row_ref[...]
    lanes = lax.broadcasted_iota(jnp.int32, row.shape, 1)
    return jnp.sum(jnp.where(lanes == position, row, 0.0), axis=1, keepdims=True)


def eye_of(size):
    rows = lax.broadcasted_iota(jnp.int32, (size, size), 0)
    cols = lax.broadcasted_iota(jnp.int32, (size, size), 1)
    return rows, cols


def three_parts(wide):
    high = wide.astype(bf16)
    rest = wide - high.astype(f32)
    mid = rest.astype(bf16)
    low = (rest - mid.astype(f32)).astype(bf16)
    return high, mid, low


def over_lanes(left, right):
    return lax.dot_general(left, right, (((1,), (1,)), ((), ())), preferred_element_type=f32)


def spread_body(vectors_ref, factors_ref, out_ref):
    unused, core = place()
    half = vectors_ref[:, pl.ds(pl.multiple_of(core * 128, 128), 128)]
    for peer in range(out_ref.shape[0]):
        out_ref[peer, :128, :] = half
        out_ref[peer, 128:144, :] = factors_ref[peer, :, :128]
        out_ref[peer, 144:160, :] = factors_ref[peer, :, 128:]


def gather_factor(got_ref, factor_ref):
    for peer in range(16):
        factor_ref[16 * peer : 16 * peer + 16, :128] = got_ref[peer, 128:144, :]
        factor_ref[16 * peer : 16 * peer + 16, 128:] = got_ref[peer, 144:160, :]


def score_body(got_ref, other_ref, centers_ref, mixing_ref, out_ref, factor_ref):
    position, core = place()
    gather_factor(got_ref, factor_ref)
    wide = factor_ref[...].astype(f32)
    center = centers_ref[pl.ds(position, 1), :]
    shifted = jnp.sum(wide * center, axis=1, keepdims=True)
    rows, cols = eye_of(256)
    diagonal = jnp.sum(jnp.where(rows == cols, wide, 0.0), axis=1, keepdims=True)
    log_diag = jnp.sum(jnp.log(diagonal), axis=0, keepdims=True)
    log_mix = jnp.log(own_of(mixing_ref, position))
    mine = factor_ref[:, pl.ds(pl.multiple_of(core * 128, 128), 128)]
    rest = factor_ref[:, pl.ds(pl.multiple_of((1 - core) * 128, 128), 128)]
    for pair in range(8):
        ours = got_ref[2 * pair : 2 * pair + 2, :128, :].reshape(256, 128)
        theirs = other_ref[2 * pair : 2 * pair + 2, :128, :].reshape(256, 128)
        whitened = over_lanes(mine, ours) + over_lanes(rest, theirs)
        whitened -= shifted
        density = log_diag - 0.5 * jnp.sum(whitened * whitened, axis=0, keepdims=True)
        scores = density + log_mix - 256 * normal_offset
        out_ref[2 * pair] = scores[:, :128]
        out_ref[2 * pair + 1] = scores[:, 128:]


def apart(left, right, **options):
    return jnp.dot(left, right, precision=exact_mode, preferred_element_type=f32)


def invert_body(got_ref, tables_ref, factor_ref, inverse_ref):
    gather_factor(got_ref, factor_ref)
    rows, cols = eye_of(128)
    factors = []
    for start in (0, 128):
        factor = factor_ref[start : start + 128, start : start + 128].astype(f32)
        diagonal = jnp.sum(jnp.where(rows == cols, factor, 0.0), axis=1, keepdims=True)
        factors.append(factor)
        inverse_ref[start // 128] = jnp.where(rows == cols, 1.0 / diagonal, 0.0)
    for level in range(7):
        below = (rows >> (level + 1) == cols >> (level + 1)) & (rows >> level > cols >> level)
        for block in range(2):
            inverse = inverse_ref[block]
            step = jnp.where(below, factors[block], 0.0)
            inverse_ref[block] = inverse - apart(apart(inverse, step), inverse)
    first, last = inverse_ref[0], inverse_ref[1]
    corner = -apart(apart(last, factor_ref[128:, :128].astype(f32)), first)
    bottom = jnp.concatenate([corner, last], axis=1)
    whole = jnp.concatenate(
        [jnp.concatenate([first, jnp.zeros((128, 128), f32)], axis=1), bottom], axis=0
    )
    square = lax.dot_general(
        whole, whole, (((1,), (1,)), ((), ())), precision=exact_mode, preferred_element_type=f32
    )
    rows, cols = eye_of(256)
    diagonal = jnp.where(rows == cols, square, 0.0)
    down = lax.rsqrt(1.0 + jnp.sum(diagonal, axis=1, keepdims=True))
    across = lax.rsqrt(1.0 + jnp.sum(diagonal, axis=0, keepdims=True))
    both = down * across
    tables = (square * both, both, jnp.where(rows == cols, across, 0.0))
    for place, table in zip((SQUARE, BOTH, START), tables):
        tables_ref[place] = table[:, :128]
        tables_ref[place + 1] = table[:, 128:]


INV_SCRATCH = [pltpu.VMEM((256, 256), bf16), pltpu.VMEM((2, 128, 128), f32)]


def order_body(got_ref, other_ref, turned_ref):
    unused, core = place()
    ours = pl.ds(pl.multiple_of(core * 128, 128), 128)
    theirs = pl.ds(pl.multiple_of((1 - core) * 128, 128), 128)
    for block in range(16):
        turned_ref[block, ours, :] = got_ref[block, :128, :].T
        turned_ref[block, theirs, :] = other_ref[block, :128, :].T


def prepare_body(got_ref, other_ref, tables_ref, turned_ref, factor_ref, inverse_ref):
    invert_body(got_ref, tables_ref, factor_ref, inverse_ref)
    order_body(got_ref, other_ref, turned_ref)


def partial_body(scores_ref, out_ref):
    scores = scores_ref[:, 0, :]
    top = jnp.max(scores, axis=0, keepdims=True)
    total = jnp.sum(jnp.exp(scores - top), axis=0, keepdims=True)
    both = jnp.concatenate([top, total], axis=0)
    for peer in range(out_ref.shape[0]):
        out_ref[peer] = both


def share_body(scores_ref, pairs_ref, shares_ref, evidence_ref):
    tops, totals = pairs_ref[:, 0, :], pairs_ref[:, 1, :]
    top = jnp.max(tops, axis=0, keepdims=True)
    total = jnp.sum(totals * jnp.exp(tops - top), axis=0, keepdims=True)
    evidence_ref[...] = top + jnp.log(total)
    shares = jnp.exp(scores_ref[:, 0, :] - top) / total
    for peer in range(shares_ref.shape[0]):
        shares_ref[peer] = shares


def same_row(tile, row):
    return jnp.broadcast_to(tile[row : row + 1, :], tile.shape)


def six_products(rows):
    high, mid, low = three_parts(rows)
    turned = jnp.concatenate([high, high, mid, high, low, mid], axis=0)
    straight = jnp.concatenate([high, mid, high, low, high, mid], axis=0)
    return turned, straight


def over_rows(left, right):
    return lax.dot_general(left, right, (((0,), (0,)), ((), ())), preferred_element_type=f32)


def eliminate(start, work_ref, tables_ref, upper_ref, out_ref):
    panel, sub = PANEL, SUB
    tiles = panel // 8
    in_tile = lax.broadcasted_iota(jnp.int32, (8, 128), 0)
    lane_of = lax.broadcasted_iota(jnp.int32, (8, 128), 1)
    far_lane = lax.broadcasted_iota(jnp.int32, (1, 128), 1)
    stop = start + panel
    near = start // 128
    rows = [
        [work_ref[start + 8 * i : start + 8 * i + 8, 128 * t : 128 * t + 128] for i in range(tiles)]
        for t in range(2)
    ]
    scale = [jnp.zeros((8, 128), f32) for i in range(tiles)]
    for begin in range(0, panel, sub):
        lane = start % 128 + begin
        columns = [
            {
                i: jnp.broadcast_to(rows[near][i][:, lane + k : lane + k + 1], (8, 128))
                for i in range((begin + k) // 8, tiles)
            }
            for k in range(sub)
        ]
        cleared = (lane_of >= lane) & (lane_of < lane + sub)
        for i in range(tiles):
            fresh = tables_ref[START + near, start + 8 * i : start + 8 * i + 8, :]
            rows[near][i] = jnp.where(cleared, fresh, rows[near][i])
        for k in range(0, sub, 2):
            row = begin + k
            tile, place = row // 8, row % 8
            one, two = columns[k], columns[k + 1]
            a, b = same_row(one[tile], place), same_row(one[tile], place + 1)
            d = same_row(two[tile], place + 1)
            root = lax.rsqrt(a * d - b * b)
            inverse = root * root
            root_a = lax.rsqrt(a)
            raw = {
                i: (one[i] * d - two[i] * b, two[i] * a - one[i] * b)
                for i in range(tile, tiles)
            }
            below = in_tile > place + 1
            raw[tile] = tuple(jnp.where(below, part, 0.0) for part in raw[tile])
            ratio = {i: (raw[i][0] * inverse, raw[i][1] * inverse) for i in raw}
            for later in range(k + 2, sub):
                other = begin + later
                f = same_row(one[other // 8], other % 8)
                g = same_row(two[other // 8], other % 8)
                for i in range(other // 8, tiles):
                    if later < k + 4:
                        change = (raw[i][0] * f + raw[i][1] * g) * inverse
                    else:
                        change = ratio[i][0] * f + ratio[i][1] * g
                    columns[later][i] = columns[later][i] - change
            ratio[tile] = (
                jnp.where(in_tile == place + 1, b * (root_a * root_a), ratio[tile][0]),
                ratio[tile][1],
            )
            for group in rows:
                f, g = same_row(group[tile], place), same_row(group[tile], place + 1)
                for i in range(tile, tiles):
                    group[i] = group[i] - (ratio[i][0] * f + ratio[i][1] * g)
            scale[tile] = jnp.where(in_tile == place, root_a, scale[tile])
            scale[tile] = jnp.where(in_tile == place + 1, root * (a * root_a), scale[tile])
    solved = [
        jnp.concatenate([group[i] * scale[i] for i in range(tiles)], axis=0) for group in rows
    ]
    for t in range(2):
        lanes = slice(128 * t, 128 * t + 128)
        done = jnp.where(far_lane + 128 * t < stop, solved[t], 0.0)
        for piece in range(panel // 16):
            out_ref[start // 16 + piece, :, lanes] = done[16 * piece : 16 * piece + 16, :]
        if near == 0:
            upper_ref[start:stop, lanes] = solved[t] if t else done
    end = 128 * near + 128
    if stop == end:
        return
    turned, straight = six_products(jnp.concatenate(solved, axis=1))
    change = over_rows(turned[:, 128 * near : end], straight)
    inside = (far_lane + 128 * near >= start) & (far_lane + 128 * near < stop)
    for t in range(2):
        lanes = slice(128 * t, 128 * t + 128)
        kept = work_ref[stop:end, lanes]
        if t == near:
            kept = jnp.where(inside, 0.0, kept)
        work_ref[stop:end, lanes] = kept - change[stop - 128 * near :, lanes]


def refactor_body(
    shares_ref, turned_ref, tables_ref, centers_ref, mixing_ref, evidence_ref,
    out_ref, far_means_ref, far_weights_ref, far_evidence_ref,
    work_ref, upper_ref, means_ref, weights_ref, sent_ref,
):
    position, unused = place()
    vector_total = turned_ref.shape[0] * turned_ref.shape[2]
    share = shares_ref[:, pl.ds(position, 1), :].reshape(16, 128)

    def weighted_parts(pair, half):
        weighted = [
            turned_ref[block, 128 * half : 128 * half + 128, :].astype(f32)
            * share[block : block + 1, :]
            for block in (2 * pair, 2 * pair + 1)
        ]
        return list(three_parts(jnp.concatenate(weighted, axis=1)))

    def vectors_of(pair, first):
        blocks = [turned_ref[block, first:, :] for block in (2 * pair, 2 * pair + 1)]
        return jnp.concatenate(blocks, axis=1)

    def added_up(parts):
        return parts[:128] + parts[128:256] + parts[256:384]

    total = jnp.zeros((432, 256), f32)
    counts = jnp.zeros((16, 128), f32)
    for pair in range(8):
        everyone = jnp.concatenate([shares_ref[2 * pair], shares_ref[2 * pair + 1]], axis=1)
        counts += everyone[:, :128] + everyone[:, 128:]
        stacked = jnp.concatenate(weighted_parts(pair, 0) + list(three_parts(everyone)), axis=0)
        total += over_lanes(stacked, vectors_of(pair, 0))
    gram = added_up(total)
    moments = total[384:400] + total[400:416] + total[416:]
    everyone_of = lax.broadcasted_iota(jnp.int32, (16, 1), 0)
    moment = jnp.sum(jnp.where(everyone_of == position, moments, 0.0), axis=0, keepdims=True)
    count = jnp.sum(jnp.sum(share, axis=0, keepdims=True), axis=1, keepdims=True)
    kept = (1.0 - step_weight) * own_of(mixing_ref, position)
    weight = kept + step_weight * count / vector_total
    center = centers_ref[pl.ds(position, 1), :]
    rows, cols = eye_of(128)
    same = rows == cols
    mean = (kept * center + step_weight * moment / vector_total) / weight

    def down(row):
        return jnp.sum(jnp.where(same, row, 0.0), axis=1, keepdims=True)

    def assembled(gram, half, t):
        mine, lanes = slice(128 * half, 128 * half + 128), slice(128 * t, 128 * t + 128)
        moment_part = (
            (kept * down(center[:, mine])) * center[:, lanes] + (step_weight / vector_total) * gram
        ) / weight - down(mean[:, mine]) * mean[:, lanes]
        if half == t:
            moment_part += jnp.where(same, ridge_term, 0.0)
        return (kept / weight) * tables_ref[SQUARE + t, mine, :] + moment_part * (
            tables_ref[BOTH + t, mine, :]
        )

    for t in range(2):
        lanes = slice(128 * t, 128 * t + 128)
        work_ref[:128, lanes] = assembled(gram[:, lanes], 0, t)
    last = jnp.zeros((384, 128), f32)
    for panel in range(128 // PANEL):
        eliminate(PANEL * panel, work_ref, tables_ref, upper_ref, out_ref)
        if panel < 2:
            for pair in range(4 * panel, 4 * panel + 4):
                stacked = jnp.concatenate(weighted_parts(pair, 1), axis=0)
                last += over_lanes(stacked, vectors_of(pair, 128))
        if panel == 0:
            few = [index[:16, :16] for index in (rows, cols)]
            everyone_at = few[0] == few[1]
            priors = jnp.sum(jnp.where(everyone_at, mixing_ref[...], 0.0), axis=1, keepdims=True)
            all_kept = (1.0 - step_weight) * priors
            counts = jnp.sum(counts, axis=1, keepdims=True)
            weights = all_kept + step_weight * counts / vector_total
            means_ref[...] = (
                all_kept * centers_ref[...] + step_weight * moments / vector_total
            ) / weights
            weights_ref[...] = jnp.sum(
                jnp.where(everyone_at, weights, 0.0), axis=0, keepdims=True
            )
        if panel == 2:
            copies = [
                pltpu.make_async_copy(source, target, sent_ref.at[place_of])
                for place_of, (source, target) in enumerate((
                    (means_ref, far_means_ref),
                    (weights_ref, far_weights_ref),
                    (evidence_ref, far_evidence_ref),
                ))
            ]
            for copy in copies:
                copy.start()
            corner = assembled(added_up(last), 1, 1)
    turned, straight = six_products(upper_ref[...])
    change = over_rows(turned[:, 128:], straight)
    work_ref[128:, :128] = -change[:, :128]
    work_ref[128:, 128:] = corner - change[:, 128:]
    for panel in range(128 // PANEL):
        eliminate(128 + PANEL * panel, work_ref, tables_ref, upper_ref, out_ref)
    for copy in copies:
        copy.wait()


REF_SCRATCH = [
    pltpu.VMEM((256, 256), f32),
    pltpu.VMEM((128, 256), f32),
    pltpu.VMEM((16, 256), f32),
    pltpu.VMEM((1, 16), f32),
    pltpu.SemaphoreType.DMA((3,)),
]


def exchanged(array, axis):
    return lax.all_to_all(array, axis, split_axis=0, concat_axis=0, tiled=True)


def local(vectors, centers, factors, mixing):
    groups, peers = lax.axis_size("dp"), lax.axis_size("comp")
    priors = mixing.reshape(1, 16)
    spread = call(spread_body, shape((groups, 160, 128), bf16), vectors, factors, near=False)
    got = exchanged(spread, "dp")
    other = lax.ppermute(got, "comp", [(i, i ^ 1) for i in range(peers)])
    scores = call(
        score_body, shape((16, 1, 128)), got, other, centers, priors,
        scratch=[pltpu.VMEM((256, 256), bf16)], flops=1 << 29,
    )
    scores, after, after_other = lax.optimization_barrier((scores, got, other))
    scores_here = exchanged(scores, "dp")
    tables, turned = call(
        prepare_body,
        [shape((TABLES, 256, 128)), shape((16, 256, 128), bf16)],
        after, after_other, scratch=INV_SCRATCH, flops=1 << 30,
    )
    scores_here, tables, turned = lax.optimization_barrier((scores_here, tables, turned))
    partial = call(partial_body, shape((peers, 2, 128)), scores_here)
    pairs = exchanged(partial, "comp")
    shares, evidence = call(
        share_body, [shape((groups, 16, 128)), shape((1, 128))], scores_here, pairs
    )
    shares_all = exchanged(shares, "dp")
    refreshed, new_means, new_weights, evidence = call(
        refactor_body, [shape((16, 16, 256)), far((16, 256)), far((1, 16)), far((1, 128))],
        shares_all, turned, tables, centers, priors, evidence, scratch=REF_SCRATCH, flops=1 << 32,
    )
    new_factors = exchanged(refreshed, "dp")
    return new_factors, new_means, new_weights.reshape(16), evidence.reshape(128)


def solution(mesh):
    return jax.shard_map(
        local,
        mesh=mesh,
        in_specs=(P("dp", None), P("comp", None), P("comp", "dp", None), P("comp")),
        out_specs=(P("comp", "dp", None), P("comp", None), P("comp"), P("dp")),
        check_vma=False,
    )
```

```python
import jax
import jax.numpy as jnp
from jax import lax
from jax.experimental import pallas as pl
from jax.experimental.pallas import tpu as pltpu
from jax.sharding import PartitionSpec as P

step_weight = 0.5
ridge_term = 0.01
normal_offset = 0.9189385332046727
exact_mode = lax.Precision.HIGHEST
PANEL = 32
SUB = 16
SQUARE, BOTH, START, TABLES = 0, 2, 4, 6
f32 = jnp.float32
bf16 = jnp.bfloat16


def call(body, out_shape, *args, scratch=(), flops=0, near=True):
    single = not isinstance(out_shape, (list, tuple))
    vmem = pl.BlockSpec(memory_space=pltpu.VMEM)
    hbm = pl.BlockSpec(memory_space=pltpu.HBM)
    space = pltpu.VMEM if near else pltpu.HBM
    args = [pltpu.with_memory_space_constraint(arg, space) for arg in args]
    return pl.pallas_call(
        body,
        out_shape=out_shape,
        in_specs=[vmem] * len(args),
        out_specs=vmem if single else [
            hbm if out.memory_space == pltpu.HBM else vmem for out in out_shape
        ],
        scratch_shapes=list(scratch),
        cost_estimate=pl.CostEstimate(flops=flops, transcendentals=0, bytes_accessed=0),
        compiler_params=pltpu.CompilerParams(vmem_limit_bytes=12 << 20),
    )(*args)


def place():
    return lax.axis_index("dp"), lax.axis_index("comp") % 2


def shape(dims, dtype=f32):
    return pltpu.VMEM(dims, dtype)


def far(dims, dtype=f32):
    return pltpu.HBM(dims, dtype)


def own_of(row_ref, position):
    row = row_ref[...]
    lanes = lax.broadcasted_iota(jnp.int32, row.shape, 1)
    return jnp.sum(jnp.where(lanes == position, row, 0.0), axis=1, keepdims=True)


def eye_of(size):
    rows = lax.broadcasted_iota(jnp.int32, (size, size), 0)
    cols = lax.broadcasted_iota(jnp.int32, (size, size), 1)
    return rows, cols


def three_parts(wide):
    high = wide.astype(bf16)
    rest = wide - high.astype(f32)
    mid = rest.astype(bf16)
    low = (rest - mid.astype(f32)).astype(bf16)
    return high, mid, low


def over_lanes(left, right):
    return lax.dot_general(left, right, (((1,), (1,)), ((), ())), preferred_element_type=f32)


def spread_body(vectors_ref, factors_ref, out_ref):
    unused, core = place()
    half = vectors_ref[:, pl.ds(pl.multiple_of(core * 128, 128), 128)]
    for peer in range(out_ref.shape[0]):
        out_ref[peer, :128, :] = half
        out_ref[peer, 128:144, :] = factors_ref[peer, :, :128]
        out_ref[peer, 144:160, :] = factors_ref[peer, :, 128:]


def gather_factor(got_ref, factor_ref):
    for peer in range(16):
        factor_ref[16 * peer : 16 * peer + 16, :128] = got_ref[peer, 128:144, :]
        factor_ref[16 * peer : 16 * peer + 16, 128:] = got_ref[peer, 144:160, :]


def score_body(got_ref, other_ref, centers_ref, mixing_ref, out_ref, factor_ref):
    position, core = place()
    gather_factor(got_ref, factor_ref)
    wide = factor_ref[...].astype(f32)
    center = centers_ref[pl.ds(position, 1), :]
    shifted = jnp.sum(wide * center, axis=1, keepdims=True)
    rows, cols = eye_of(256)
    diagonal = jnp.sum(jnp.where(rows == cols, wide, 0.0), axis=1, keepdims=True)
    log_diag = jnp.sum(jnp.log(diagonal), axis=0, keepdims=True)
    log_mix = jnp.log(own_of(mixing_ref, position))
    mine = factor_ref[:, pl.ds(pl.multiple_of(core * 128, 128), 128)]
    rest = factor_ref[:, pl.ds(pl.multiple_of((1 - core) * 128, 128), 128)]
    for pair in range(8):
        ours = got_ref[2 * pair : 2 * pair + 2, :128, :].reshape(256, 128)
        theirs = other_ref[2 * pair : 2 * pair + 2, :128, :].reshape(256, 128)
        whitened = over_lanes(mine, ours) + over_lanes(rest, theirs)
        whitened -= shifted
        density = log_diag - 0.5 * jnp.sum(whitened * whitened, axis=0, keepdims=True)
        scores = density + log_mix - 256 * normal_offset
        out_ref[2 * pair] = scores[:, :128]
        out_ref[2 * pair + 1] = scores[:, 128:]


def apart(left, right, **options):
    return jnp.dot(left, right, precision=exact_mode, preferred_element_type=f32)


def invert_body(got_ref, tables_ref, factor_ref, inverse_ref):
    gather_factor(got_ref, factor_ref)
    rows, cols = eye_of(128)
    factors = []
    for start in (0, 128):
        factor = factor_ref[start : start + 128, start : start + 128].astype(f32)
        diagonal = jnp.sum(jnp.where(rows == cols, factor, 0.0), axis=1, keepdims=True)
        factors.append(factor)
        inverse_ref[start // 128] = jnp.where(rows == cols, 1.0 / diagonal, 0.0)
    for level in range(7):
        below = (rows >> (level + 1) == cols >> (level + 1)) & (rows >> level > cols >> level)
        for block in range(2):
            inverse = inverse_ref[block]
            step = jnp.where(below, factors[block], 0.0)
            inverse_ref[block] = inverse - apart(apart(inverse, step), inverse)
    first, last = inverse_ref[0], inverse_ref[1]
    corner = -apart(apart(last, factor_ref[128:, :128].astype(f32)), first)
    bottom = jnp.concatenate([corner, last], axis=1)
    whole = jnp.concatenate(
        [jnp.concatenate([first, jnp.zeros((128, 128), f32)], axis=1), bottom], axis=0
    )
    square = lax.dot_general(
        whole, whole, (((1,), (1,)), ((), ())), precision=exact_mode, preferred_element_type=f32
    )
    rows, cols = eye_of(256)
    diagonal = jnp.where(rows == cols, square, 0.0)
    down = lax.rsqrt(1.0 + jnp.sum(diagonal, axis=1, keepdims=True))
    across = lax.rsqrt(1.0 + jnp.sum(diagonal, axis=0, keepdims=True))
    both = down * across
    tables = (square * both, both, jnp.where(rows == cols, across, 0.0))
    for place, table in zip((SQUARE, BOTH, START), tables):
        tables_ref[place] = table[:, :128]
        tables_ref[place + 1] = table[:, 128:]


INV_SCRATCH = [pltpu.VMEM((256, 256), bf16), pltpu.VMEM((2, 128, 128), f32)]


def order_body(got_ref, other_ref, turned_ref):
    unused, core = place()
    ours = pl.ds(pl.multiple_of(core * 128, 128), 128)
    theirs = pl.ds(pl.multiple_of((1 - core) * 128, 128), 128)
    for block in range(16):
        turned_ref[block, ours, :] = got_ref[block, :128, :].T
        turned_ref[block, theirs, :] = other_ref[block, :128, :].T


def prepare_body(got_ref, other_ref, tables_ref, turned_ref, factor_ref, inverse_ref):
    invert_body(got_ref, tables_ref, factor_ref, inverse_ref)
    order_body(got_ref, other_ref, turned_ref)


def partial_body(scores_ref, out_ref):
    scores = scores_ref[:, 0, :]
    top = jnp.max(scores, axis=0, keepdims=True)
    total = jnp.sum(jnp.exp(scores - top), axis=0, keepdims=True)
    both = jnp.concatenate([top, total], axis=0)
    for peer in range(out_ref.shape[0]):
        out_ref[peer] = both


def share_body(scores_ref, pairs_ref, shares_ref, evidence_ref):
    tops, totals = pairs_ref[:, 0, :], pairs_ref[:, 1, :]
    top = jnp.max(tops, axis=0, keepdims=True)
    total = jnp.sum(totals * jnp.exp(tops - top), axis=0, keepdims=True)
    evidence_ref[...] = top + jnp.log(total)
    shares = jnp.exp(scores_ref[:, 0, :] - top) / total
    for peer in range(shares_ref.shape[0]):
        shares_ref[peer] = shares


def same_row(tile, row):
    return jnp.broadcast_to(tile[row : row + 1, :], tile.shape)


def six_products(rows):
    high, mid, low = three_parts(rows)
    turned = jnp.concatenate([high, high, mid, high, low, mid], axis=0)
    straight = jnp.concatenate([high, mid, high, low, high, mid], axis=0)
    return turned, straight


def over_rows(left, right):
    return lax.dot_general(left, right, (((0,), (0,)), ((), ())), preferred_element_type=f32)


def eliminate(start, work_ref, tables_ref, upper_ref, out_ref):
    panel, sub = PANEL, SUB
    tiles = panel // 8
    in_tile = lax.broadcasted_iota(jnp.int32, (8, 128), 0)
    lane_of = lax.broadcasted_iota(jnp.int32, (8, 128), 1)
    far_lane = lax.broadcasted_iota(jnp.int32, (1, 128), 1)
    stop = start + panel
    near = start // 128
    rows = [
        [work_ref[start + 8 * i : start + 8 * i + 8, 128 * t : 128 * t + 128] for i in range(tiles)]
        for t in range(2)
    ]
    scale = [jnp.zeros((8, 128), f32) for i in range(tiles)]
    for begin in range(0, panel, sub):
        lane = start % 128 + begin
        columns = [
            {
                i: jnp.broadcast_to(rows[near][i][:, lane + k : lane + k + 1], (8, 128))
                for i in range((begin + k) // 8, tiles)
            }
            for k in range(sub)
        ]
        cleared = (lane_of >= lane) & (lane_of < lane + sub)
        for i in range(tiles):
            fresh = tables_ref[START + near, start + 8 * i : start + 8 * i + 8, :]
            rows[near][i] = jnp.where(cleared, fresh, rows[near][i])
        for k in range(0, sub, 2):
            row = begin + k
            tile, place = row // 8, row % 8
            one, two = columns[k], columns[k + 1]
            a, b = same_row(one[tile], place), same_row(one[tile], place + 1)
            d = same_row(two[tile], place + 1)
            root = lax.rsqrt(a * d - b * b)
            inverse = root * root
            root_a = lax.rsqrt(a)
            raw = {
                i: (one[i] * d - two[i] * b, two[i] * a - one[i] * b)
                for i in range(tile, tiles)
            }
            below = in_tile > place + 1
            raw[tile] = tuple(jnp.where(below, part, 0.0) for part in raw[tile])
            ratio = {i: (raw[i][0] * inverse, raw[i][1] * inverse) for i in raw}
            for later in range(k + 2, sub):
                other = begin + later
                f = same_row(one[other // 8], other % 8)
                g = same_row(two[other // 8], other % 8)
                for i in range(other // 8, tiles):
                    if later < k + 4:
                        change = (raw[i][0] * f + raw[i][1] * g) * inverse
                    else:
                        change = ratio[i][0] * f + ratio[i][1] * g
                    columns[later][i] = columns[later][i] - change
            ratio[tile] = (
                jnp.where(in_tile == place + 1, b * (root_a * root_a), ratio[tile][0]),
                ratio[tile][1],
            )
            for group in rows:
                f, g = same_row(group[tile], place), same_row(group[tile], place + 1)
                for i in range(tile, tiles):
                    group[i] = group[i] - (ratio[i][0] * f + ratio[i][1] * g)
            scale[tile] = jnp.where(in_tile == place, root_a, scale[tile])
            scale[tile] = jnp.where(in_tile == place + 1, root * (a * root_a), scale[tile])
    solved = [
        jnp.concatenate([group[i] * scale[i] for i in range(tiles)], axis=0) for group in rows
    ]
    for t in range(2):
        lanes = slice(128 * t, 128 * t + 128)
        done = jnp.where(far_lane + 128 * t < stop, solved[t], 0.0)
        for piece in range(panel // 16):
            out_ref[start // 16 + piece, :, lanes] = done[16 * piece : 16 * piece + 16, :]
        if near == 0:
            upper_ref[start:stop, lanes] = solved[t] if t else done
    end = 128 * near + 128
    if stop == end:
        return
    turned, straight = six_products(jnp.concatenate(solved, axis=1))
    change = over_rows(turned[:, 128 * near : end], straight)
    inside = (far_lane + 128 * near >= start) & (far_lane + 128 * near < stop)
    for t in range(2):
        lanes = slice(128 * t, 128 * t + 128)
        kept = work_ref[stop:end, lanes]
        if t == near:
            kept = jnp.where(inside, 0.0, kept)
        work_ref[stop:end, lanes] = kept - change[stop - 128 * near :, lanes]


def refactor_body(
    shares_ref, turned_ref, tables_ref, centers_ref, mixing_ref,
    out_ref, means_ref, weights_ref, work_ref, upper_ref,
):
    position, unused = place()
    vector_total = turned_ref.shape[0] * turned_ref.shape[2]
    share = shares_ref[:, pl.ds(position, 1), :].reshape(16, 128)

    def weighted_parts(pair, half):
        weighted = [
            turned_ref[block, 128 * half : 128 * half + 128, :].astype(f32)
            * share[block : block + 1, :]
            for block in (2 * pair, 2 * pair + 1)
        ]
        return list(three_parts(jnp.concatenate(weighted, axis=1)))

    def vectors_of(pair, first):
        blocks = [turned_ref[block, first:, :] for block in (2 * pair, 2 * pair + 1)]
        return jnp.concatenate(blocks, axis=1)

    def added_up(parts):
        return parts[:128] + parts[128:256] + parts[256:384]

    total = jnp.zeros((432, 256), f32)
    counts = jnp.zeros((16, 128), f32)
    for pair in range(8):
        everyone = jnp.concatenate([shares_ref[2 * pair], shares_ref[2 * pair + 1]], axis=1)
        counts += everyone[:, :128] + everyone[:, 128:]
        stacked = jnp.concatenate(weighted_parts(pair, 0) + list(three_parts(everyone)), axis=0)
        total += over_lanes(stacked, vectors_of(pair, 0))
    gram = added_up(total)
    moments = total[384:400] + total[400:416] + total[416:]
    everyone_of = lax.broadcasted_iota(jnp.int32, (16, 1), 0)
    moment = jnp.sum(jnp.where(everyone_of == position, moments, 0.0), axis=0, keepdims=True)
    count = jnp.sum(jnp.sum(share, axis=0, keepdims=True), axis=1, keepdims=True)
    kept = (1.0 - step_weight) * own_of(mixing_ref, position)
    weight = kept + step_weight * count / vector_total
    center = centers_ref[pl.ds(position, 1), :]
    rows, cols = eye_of(128)
    same = rows == cols
    mean = (kept * center + step_weight * moment / vector_total) / weight

    def down(row):
        return jnp.sum(jnp.where(same, row, 0.0), axis=1, keepdims=True)

    def assembled(gram, half, t):
        mine, lanes = slice(128 * half, 128 * half + 128), slice(128 * t, 128 * t + 128)
        moment_part = (
            (kept * down(center[:, mine])) * center[:, lanes] + (step_weight / vector_total) * gram
        ) / weight - down(mean[:, mine]) * mean[:, lanes]
        if half == t:
            moment_part += jnp.where(same, ridge_term, 0.0)
        return (kept / weight) * tables_ref[SQUARE + t, mine, :] + moment_part * (
            tables_ref[BOTH + t, mine, :]
        )

    for t in range(2):
        lanes = slice(128 * t, 128 * t + 128)
        work_ref[:128, lanes] = assembled(gram[:, lanes], 0, t)
    last = jnp.zeros((384, 128), f32)
    for panel in range(128 // PANEL):
        eliminate(PANEL * panel, work_ref, tables_ref, upper_ref, out_ref)
        if panel < 2:
            for pair in range(4 * panel, 4 * panel + 4):
                stacked = jnp.concatenate(weighted_parts(pair, 1), axis=0)
                last += over_lanes(stacked, vectors_of(pair, 128))
        if panel == 0:
            few = [index[:16, :16] for index in (rows, cols)]
            everyone_at = few[0] == few[1]
            priors = jnp.sum(jnp.where(everyone_at, mixing_ref[...], 0.0), axis=1, keepdims=True)
            all_kept = (1.0 - step_weight) * priors
            counts = jnp.sum(counts, axis=1, keepdims=True)
            weights = all_kept + step_weight * counts / vector_total
            means_ref[...] = (
                all_kept * centers_ref[...] + step_weight * moments / vector_total
            ) / weights
            weights_ref[...] = jnp.sum(
                jnp.where(everyone_at, weights, 0.0), axis=0, keepdims=True
            )
        if panel == 2:
            corner = assembled(added_up(last), 1, 1)
    turned, straight = six_products(upper_ref[...])
    change = over_rows(turned[:, 128:], straight)
    work_ref[128:, :128] = -change[:, :128]
    work_ref[128:, 128:] = corner - change[:, 128:]
    for panel in range(128 // PANEL):
        eliminate(128 + PANEL * panel, work_ref, tables_ref, upper_ref, out_ref)


REF_SCRATCH = [
    pltpu.VMEM((256, 256), f32),
    pltpu.VMEM((128, 256), f32),
]


def close_body(*refs):
    sources, targets, sent_ref = refs[:4], refs[4:8], refs[8]
    copies = []
    for source, target in zip(sources[1:], targets[1:]):
        copies.append((source, target))
    for part in range(4):
        copies.append((sources[0].at[4 * part : 4 * part + 4], targets[0].at[4 * part : 4 * part + 4]))
    copies = [
        pltpu.make_async_copy(source, target, sent_ref.at[place_of])
        for place_of, (source, target) in enumerate(copies)
    ]
    for copy in copies:
        copy.start()
    for copy in copies:
        copy.wait()


def exchanged(array, axis):
    return lax.all_to_all(array, axis, split_axis=0, concat_axis=0, tiled=True)


def local(vectors, centers, factors, mixing):
    groups, peers = lax.axis_size("dp"), lax.axis_size("comp")
    priors = mixing.reshape(1, 16)
    spread = call(spread_body, shape((groups, 160, 128), bf16), vectors, factors, near=False)
    got = exchanged(spread, "dp")
    other = lax.ppermute(got, "comp", [(i, i ^ 1) for i in range(peers)])
    scores = call(
        score_body, shape((16, 1, 128)), got, other, centers, priors,
        scratch=[pltpu.VMEM((256, 256), bf16)], flops=1 << 29,
    )
    scores, after, after_other = lax.optimization_barrier((scores, got, other))
    scores_here = exchanged(scores, "dp")
    tables, turned = call(
        prepare_body,
        [shape((TABLES, 256, 128)), shape((16, 256, 128), bf16)],
        after, after_other, scratch=INV_SCRATCH, flops=1 << 30,
    )
    scores_here, tables, turned = lax.optimization_barrier((scores_here, tables, turned))
    partial = call(partial_body, shape((peers, 2, 128)), scores_here)
    pairs = exchanged(partial, "comp")
    shares, evidence = call(
        share_body, [shape((groups, 16, 128)), shape((1, 128))], scores_here, pairs
    )
    shares_all = exchanged(shares, "dp")
    refreshed, new_means, new_weights = call(
        refactor_body, [shape((16, 16, 256)), shape((16, 256)), shape((1, 16))],
        shares_all, turned, tables, centers, priors, scratch=REF_SCRATCH, flops=1 << 32,
    )
    new_factors, new_means, new_weights, evidence = call(
        close_body, [far((16, 16, 256)), far((16, 256)), far((1, 16)), far((1, 128))],
        exchanged(refreshed, "dp"), new_means, new_weights, evidence,
        scratch=[pltpu.SemaphoreType.DMA((7,))],
    )
    return new_factors, new_means, new_weights.reshape(16), evidence.reshape(128)


def solution(mesh):
    return jax.shard_map(
        local,
        mesh=mesh,
        in_specs=(P("dp", None), P("comp", None), P("comp", "dp", None), P("comp")),
        out_specs=(P("comp", "dp", None), P("comp", None), P("comp"), P("dp")),
        check_vma=False,
    )
```

```python
import jax
import jax.numpy as jnp
from jax import lax
from jax.experimental import pallas as pl
from jax.experimental.pallas import tpu as pltpu
from jax.sharding import PartitionSpec as P

step_weight = 0.5
ridge_term = 0.01
normal_offset = 0.9189385332046727
exact_mode = lax.Precision.HIGHEST
PANEL = 32
SUB = 16
SQUARE, BOTH, START, TABLES = 0, 2, 4, 6
f32 = jnp.float32
bf16 = jnp.bfloat16


def call(body, out_shape, *args, scratch=(), flops=0, near=True):
    single = not isinstance(out_shape, (list, tuple))
    vmem = pl.BlockSpec(memory_space=pltpu.VMEM)
    hbm = pl.BlockSpec(memory_space=pltpu.HBM)
    space = pltpu.VMEM if near else pltpu.HBM
    args = [pltpu.with_memory_space_constraint(arg, space) for arg in args]
    return pl.pallas_call(
        body,
        out_shape=out_shape,
        in_specs=[vmem] * len(args),
        out_specs=vmem if single else [
            hbm if out.memory_space == pltpu.HBM else vmem for out in out_shape
        ],
        scratch_shapes=list(scratch),
        cost_estimate=pl.CostEstimate(flops=flops, transcendentals=0, bytes_accessed=0),
        compiler_params=pltpu.CompilerParams(vmem_limit_bytes=12 << 20),
    )(*args)


def place():
    return lax.axis_index("dp"), lax.axis_index("comp") % 2


def shape(dims, dtype=f32):
    return pltpu.VMEM(dims, dtype)


def far(dims, dtype=f32):
    return pltpu.HBM(dims, dtype)


def own_of(row_ref, position):
    row = row_ref[...]
    lanes = lax.broadcasted_iota(jnp.int32, row.shape, 1)
    return jnp.sum(jnp.where(lanes == position, row, 0.0), axis=1, keepdims=True)


def eye_of(size):
    rows = lax.broadcasted_iota(jnp.int32, (size, size), 0)
    cols = lax.broadcasted_iota(jnp.int32, (size, size), 1)
    return rows, cols


def three_parts(wide):
    high = wide.astype(bf16)
    rest = wide - high.astype(f32)
    mid = rest.astype(bf16)
    low = (rest - mid.astype(f32)).astype(bf16)
    return high, mid, low


def over_lanes(left, right):
    return lax.dot_general(left, right, (((1,), (1,)), ((), ())), preferred_element_type=f32)


def spread_body(vectors_ref, factors_ref, out_ref):
    unused, core = place()
    half = vectors_ref[:, pl.ds(pl.multiple_of(core * 128, 128), 128)]
    for peer in range(out_ref.shape[0]):
        out_ref[peer, :128, :] = half
        out_ref[peer, 128:144, :] = factors_ref[peer, :, :128]
        out_ref[peer, 144:160, :] = factors_ref[peer, :, 128:]


def gather_factor(got_ref, factor_ref):
    for peer in range(16):
        factor_ref[16 * peer : 16 * peer + 16, :128] = got_ref[peer, 128:144, :]
        factor_ref[16 * peer : 16 * peer + 16, 128:] = got_ref[peer, 144:160, :]


def factor_body(got_ref, centers_ref, mixing_ref, factor_ref, shifted_ref, constant_ref):
    position, unused = place()
    gather_factor(got_ref, factor_ref)
    wide = factor_ref[...].astype(f32)
    center = centers_ref[pl.ds(position, 1), :]
    shifted = jnp.sum(wide * center, axis=1, keepdims=True)
    shifted_ref[...] = jnp.broadcast_to(shifted, (256, 128))
    rows, cols = eye_of(256)
    diagonal = jnp.sum(jnp.where(rows == cols, wide, 0.0), axis=1, keepdims=True)
    log_diag = jnp.sum(jnp.log(diagonal), axis=0, keepdims=True)
    log_mix = jnp.log(own_of(mixing_ref, position))
    constant_ref[0:1, :] = jnp.broadcast_to(log_diag, (1, 128))
    constant_ref[1:2, :] = jnp.broadcast_to(log_mix, (1, 128))


def score_body(got_ref, other_ref, factor_ref, shifted_ref, constant_ref, out_ref):
    unused, core = place()
    mine = factor_ref[:, pl.ds(pl.multiple_of(core * 128, 128), 128)]
    rest = factor_ref[:, pl.ds(pl.multiple_of((1 - core) * 128, 128), 128)]
    for pair in range(8):
        ours = got_ref[2 * pair : 2 * pair + 2, :128, :].reshape(256, 128)
        theirs = other_ref[2 * pair : 2 * pair + 2, :128, :].reshape(256, 128)
        product = over_lanes(mine, ours) + over_lanes(rest, theirs)
        for block in range(2):
            whitened = product[:, 128 * block : 128 * block + 128] - shifted_ref[...]
            density = constant_ref[0:1, :] - 0.5 * jnp.sum(
                whitened * whitened, axis=0, keepdims=True
            )
            out_ref[2 * pair + block] = density + constant_ref[1:2, :] - 256 * normal_offset


def apart(left, right, **options):
    return jnp.dot(left, right, precision=exact_mode, preferred_element_type=f32)


def invert_body(factor_ref, tables_ref, inverse_ref):
    rows, cols = eye_of(128)
    factors = []
    for start in (0, 128):
        factor = factor_ref[start : start + 128, start : start + 128].astype(f32)
        diagonal = jnp.sum(jnp.where(rows == cols, factor, 0.0), axis=1, keepdims=True)
        factors.append(factor)
        inverse_ref[start // 128] = jnp.where(rows == cols, 1.0 / diagonal, 0.0)
    for level in range(7):
        below = (rows >> (level + 1) == cols >> (level + 1)) & (rows >> level > cols >> level)
        for block in range(2):
            inverse = inverse_ref[block]
            step = jnp.where(below, factors[block], 0.0)
            inverse_ref[block] = inverse - apart(apart(inverse, step), inverse)
    first, last = inverse_ref[0], inverse_ref[1]
    corner = -apart(apart(last, factor_ref[128:, :128].astype(f32)), first)
    bottom = jnp.concatenate([corner, last], axis=1)
    whole = jnp.concatenate(
        [jnp.concatenate([first, jnp.zeros((128, 128), f32)], axis=1), bottom], axis=0
    )
    square = lax.dot_general(
        whole, whole, (((1,), (1,)), ((), ())), precision=exact_mode, preferred_element_type=f32
    )
    rows, cols = eye_of(256)
    diagonal = jnp.where(rows == cols, square, 0.0)
    down = lax.rsqrt(1.0 + jnp.sum(diagonal, axis=1, keepdims=True))
    across = lax.rsqrt(1.0 + jnp.sum(diagonal, axis=0, keepdims=True))
    both = down * across
    tables = (square * both, both, jnp.where(rows == cols, across, 0.0))
    for place, table in zip((SQUARE, BOTH, START), tables):
        tables_ref[place] = table[:, :128]
        tables_ref[place + 1] = table[:, 128:]


INV_SCRATCH = [pltpu.VMEM((2, 128, 128), f32)]


def order_body(got_ref, other_ref, turned_ref):
    unused, core = place()
    ours = pl.ds(pl.multiple_of(core * 128, 128), 128)
    theirs = pl.ds(pl.multiple_of((1 - core) * 128, 128), 128)
    for block in range(16):
        turned_ref[block, ours, :] = got_ref[block, :128, :].T
        turned_ref[block, theirs, :] = other_ref[block, :128, :].T


def prepare_body(got_ref, other_ref, factor_ref, tables_ref, turned_ref, inverse_ref):
    invert_body(factor_ref, tables_ref, inverse_ref)
    order_body(got_ref, other_ref, turned_ref)


def partial_body(scores_ref, out_ref):
    scores = scores_ref[:, 0, :]
    top = jnp.max(scores, axis=0, keepdims=True)
    total = jnp.sum(jnp.exp(scores - top), axis=0, keepdims=True)
    both = jnp.concatenate([top, total], axis=0)
    for peer in range(out_ref.shape[0]):
        out_ref[peer] = both


def share_body(scores_ref, pairs_ref, shares_ref, evidence_ref):
    tops, totals = pairs_ref[:, 0, :], pairs_ref[:, 1, :]
    top = jnp.max(tops, axis=0, keepdims=True)
    total = jnp.sum(totals * jnp.exp(tops - top), axis=0, keepdims=True)
    evidence_ref[...] = top + jnp.log(total)
    shares = jnp.exp(scores_ref[:, 0, :] - top) / total
    for peer in range(shares_ref.shape[0]):
        shares_ref[peer] = shares


def same_row(tile, row):
    return jnp.broadcast_to(tile[row : row + 1, :], tile.shape)


def six_products(rows):
    high, mid, low = three_parts(rows)
    turned = jnp.concatenate([high, high, mid, high, low, mid], axis=0)
    straight = jnp.concatenate([high, mid, high, low, high, mid], axis=0)
    return turned, straight


def over_rows(left, right):
    return lax.dot_general(left, right, (((0,), (0,)), ((), ())), preferred_element_type=f32)


def eliminate(start, work_ref, tables_ref, upper_ref, out_ref):
    panel, sub = PANEL, SUB
    tiles = panel // 8
    in_tile = lax.broadcasted_iota(jnp.int32, (8, 128), 0)
    lane_of = lax.broadcasted_iota(jnp.int32, (8, 128), 1)
    far_lane = lax.broadcasted_iota(jnp.int32, (1, 128), 1)
    stop = start + panel
    near = start // 128
    rows = [
        [work_ref[start + 8 * i : start + 8 * i + 8, 128 * t : 128 * t + 128] for i in range(tiles)]
        for t in range(2)
    ]
    scale = [jnp.zeros((8, 128), f32) for i in range(tiles)]
    for begin in range(0, panel, sub):
        lane = start % 128 + begin
        columns = [
            {
                i: jnp.broadcast_to(rows[near][i][:, lane + k : lane + k + 1], (8, 128))
                for i in range((begin + k) // 8, tiles)
            }
            for k in range(sub)
        ]
        cleared = (lane_of >= lane) & (lane_of < lane + sub)
        for i in range(tiles):
            fresh = tables_ref[START + near, start + 8 * i : start + 8 * i + 8, :]
            rows[near][i] = jnp.where(cleared, fresh, rows[near][i])
        for k in range(0, sub, 2):
            row = begin + k
            tile, place = row // 8, row % 8
            one, two = columns[k], columns[k + 1]
            a, b = same_row(one[tile], place), same_row(one[tile], place + 1)
            d = same_row(two[tile], place + 1)
            root = lax.rsqrt(a * d - b * b)
            inverse = root * root
            root_a = lax.rsqrt(a)
            raw = {
                i: (one[i] * d - two[i] * b, two[i] * a - one[i] * b)
                for i in range(tile, tiles)
            }
            below = in_tile > place + 1
            raw[tile] = tuple(jnp.where(below, part, 0.0) for part in raw[tile])
            ratio = {i: (raw[i][0] * inverse, raw[i][1] * inverse) for i in raw}
            for later in range(k + 2, sub):
                other = begin + later
                f = same_row(one[other // 8], other % 8)
                g = same_row(two[other // 8], other % 8)
                for i in range(other // 8, tiles):
                    if later < k + 4:
                        change = (raw[i][0] * f + raw[i][1] * g) * inverse
                    else:
                        change = ratio[i][0] * f + ratio[i][1] * g
                    columns[later][i] = columns[later][i] - change
            ratio[tile] = (
                jnp.where(in_tile == place + 1, b * (root_a * root_a), ratio[tile][0]),
                ratio[tile][1],
            )
            for group in rows:
                f, g = same_row(group[tile], place), same_row(group[tile], place + 1)
                for i in range(tile, tiles):
                    group[i] = group[i] - (ratio[i][0] * f + ratio[i][1] * g)
            scale[tile] = jnp.where(in_tile == place, root_a, scale[tile])
            scale[tile] = jnp.where(in_tile == place + 1, root * (a * root_a), scale[tile])
    solved = [
        jnp.concatenate([group[i] * scale[i] for i in range(tiles)], axis=0) for group in rows
    ]
    for t in range(2):
        lanes = slice(128 * t, 128 * t + 128)
        done = jnp.where(far_lane + 128 * t < stop, solved[t], 0.0)
        for piece in range(panel // 16):
            out_ref[start // 16 + piece, :, lanes] = done[16 * piece : 16 * piece + 16, :]
        if near == 0:
            upper_ref[start:stop, lanes] = solved[t] if t else done
    end = 128 * near + 128
    if stop == end:
        return
    turned, straight = six_products(jnp.concatenate(solved, axis=1))
    change = over_rows(turned[:, 128 * near : end], straight)
    inside = (far_lane + 128 * near >= start) & (far_lane + 128 * near < stop)
    for t in range(2):
        lanes = slice(128 * t, 128 * t + 128)
        kept = work_ref[stop:end, lanes]
        if t == near:
            kept = jnp.where(inside, 0.0, kept)
        work_ref[stop:end, lanes] = kept - change[stop - 128 * near :, lanes]


def refactor_body(
    shares_ref, turned_ref, tables_ref, centers_ref, mixing_ref,
    out_ref, means_ref, weights_ref, work_ref, upper_ref,
):
    position, unused = place()
    vector_total = turned_ref.shape[0] * turned_ref.shape[2]
    share = shares_ref[:, pl.ds(position, 1), :].reshape(16, 128)

    def weighted_parts(pair, half):
        weighted = [
            turned_ref[block, 128 * half : 128 * half + 128, :].astype(f32)
            * share[block : block + 1, :]
            for block in (2 * pair, 2 * pair + 1)
        ]
        return list(three_parts(jnp.concatenate(weighted, axis=1)))

    def vectors_of(pair, first):
        blocks = [turned_ref[block, first:, :] for block in (2 * pair, 2 * pair + 1)]
        return jnp.concatenate(blocks, axis=1)

    def added_up(parts):
        return parts[:128] + parts[128:256] + parts[256:384]

    total = jnp.zeros((432, 256), f32)
    counts = jnp.zeros((16, 128), f32)
    for pair in range(8):
        everyone = jnp.concatenate([shares_ref[2 * pair], shares_ref[2 * pair + 1]], axis=1)
        counts += everyone[:, :128] + everyone[:, 128:]
        stacked = jnp.concatenate(weighted_parts(pair, 0) + list(three_parts(everyone)), axis=0)
        total += over_lanes(stacked, vectors_of(pair, 0))
    gram = added_up(total)
    moments = total[384:400] + total[400:416] + total[416:]
    everyone_of = lax.broadcasted_iota(jnp.int32, (16, 1), 0)
    moment = jnp.sum(jnp.where(everyone_of == position, moments, 0.0), axis=0, keepdims=True)
    count = jnp.sum(jnp.sum(share, axis=0, keepdims=True), axis=1, keepdims=True)
    kept = (1.0 - step_weight) * own_of(mixing_ref, position)
    weight = kept + step_weight * count / vector_total
    center = centers_ref[pl.ds(position, 1), :]
    rows, cols = eye_of(128)
    same = rows == cols
    mean = (kept * center + step_weight * moment / vector_total) / weight

    def down(row):
        return jnp.sum(jnp.where(same, row, 0.0), axis=1, keepdims=True)

    def assembled(gram, half, t):
        mine, lanes = slice(128 * half, 128 * half + 128), slice(128 * t, 128 * t + 128)
        moment_part = (
            (kept * down(center[:, mine])) * center[:, lanes] + (step_weight / vector_total) * gram
        ) / weight - down(mean[:, mine]) * mean[:, lanes]
        if half == t:
            moment_part += jnp.where(same, ridge_term, 0.0)
        return (kept / weight) * tables_ref[SQUARE + t, mine, :] + moment_part * (
            tables_ref[BOTH + t, mine, :]
        )

    for t in range(2):
        lanes = slice(128 * t, 128 * t + 128)
        work_ref[:128, lanes] = assembled(gram[:, lanes], 0, t)
    last = jnp.zeros((384, 128), f32)
    for panel in range(128 // PANEL):
        eliminate(PANEL * panel, work_ref, tables_ref, upper_ref, out_ref)
        if panel < 2:
            for pair in range(4 * panel, 4 * panel + 4):
                stacked = jnp.concatenate(weighted_parts(pair, 1), axis=0)
                last += over_lanes(stacked, vectors_of(pair, 128))
        if panel == 0:
            few = [index[:16, :16] for index in (rows, cols)]
            everyone_at = few[0] == few[1]
            priors = jnp.sum(jnp.where(everyone_at, mixing_ref[...], 0.0), axis=1, keepdims=True)
            all_kept = (1.0 - step_weight) * priors
            counts = jnp.sum(counts, axis=1, keepdims=True)
            weights = all_kept + step_weight * counts / vector_total
            means_ref[...] = (
                all_kept * centers_ref[...] + step_weight * moments / vector_total
            ) / weights
            weights_ref[...] = jnp.sum(
                jnp.where(everyone_at, weights, 0.0), axis=0, keepdims=True
            )
        if panel == 2:
            corner = assembled(added_up(last), 1, 1)
    turned, straight = six_products(upper_ref[...])
    change = over_rows(turned[:, 128:], straight)
    work_ref[128:, :128] = -change[:, :128]
    work_ref[128:, 128:] = corner - change[:, 128:]
    for panel in range(128 // PANEL):
        eliminate(128 + PANEL * panel, work_ref, tables_ref, upper_ref, out_ref)


REF_SCRATCH = [
    pltpu.VMEM((256, 256), f32),
    pltpu.VMEM((128, 256), f32),
]


def close_body(*refs):
    sources, targets, sent_ref = refs[:4], refs[4:8], refs[8]
    copies = []
    for source, target in zip(sources[1:], targets[1:]):
        copies.append((source, target))
    for part in range(4):
        copies.append((sources[0].at[4 * part : 4 * part + 4], targets[0].at[4 * part : 4 * part + 4]))
    copies = [
        pltpu.make_async_copy(source, target, sent_ref.at[place_of])
        for place_of, (source, target) in enumerate(copies)
    ]
    for copy in copies:
        copy.start()
    for copy in copies:
        copy.wait()


def exchanged(array, axis):
    return lax.all_to_all(array, axis, split_axis=0, concat_axis=0, tiled=True)


def local(vectors, centers, factors, mixing):
    groups, peers = lax.axis_size("dp"), lax.axis_size("comp")
    priors = mixing.reshape(1, 16)
    spread = call(spread_body, shape((groups, 160, 128), bf16), vectors, factors, near=False)
    got = exchanged(spread, "dp")
    other = lax.ppermute(got, "comp", [(i, i ^ 1) for i in range(peers)])
    factor, shifted, constant = call(
        factor_body, [shape((256, 256), bf16), shape((256, 128)), shape((2, 128))],
        got, centers, priors, flops=1 << 27,
    )
    scores = call(
        score_body, shape((16, 1, 128)), got, other, factor, shifted, constant, flops=1 << 29,
    )
    scores, after, after_other = lax.optimization_barrier((scores, got, other))
    scores_here = exchanged(scores, "dp")
    tables, turned = call(
        prepare_body,
        [shape((TABLES, 256, 128)), shape((16, 256, 128), bf16)],
        after, after_other, factor, scratch=INV_SCRATCH, flops=1 << 30,
    )
    scores_here, tables, turned = lax.optimization_barrier((scores_here, tables, turned))
    partial = call(partial_body, shape((peers, 2, 128)), scores_here)
    pairs = exchanged(partial, "comp")
    shares, evidence = call(
        share_body, [shape((groups, 16, 128)), shape((1, 128))], scores_here, pairs
    )
    shares_all = exchanged(shares, "dp")
    refreshed, new_means, new_weights = call(
        refactor_body, [shape((16, 16, 256)), shape((16, 256)), shape((1, 16))],
        shares_all, turned, tables, centers, priors, scratch=REF_SCRATCH, flops=1 << 32,
    )
    new_factors, new_means, new_weights, evidence = call(
        close_body, [far((16, 16, 256)), far((16, 256)), far((1, 16)), far((1, 128))],
        exchanged(refreshed, "dp"), new_means, new_weights, evidence,
        scratch=[pltpu.SemaphoreType.DMA((7,))],
    )
    return new_factors, new_means, new_weights.reshape(16), evidence.reshape(128)


def solution(mesh):
    return jax.shard_map(
        local,
        mesh=mesh,
        in_specs=(P("dp", None), P("comp", None), P("comp", "dp", None), P("comp")),
        out_specs=(P("comp", "dp", None), P("comp", None), P("comp"), P("dp")),
        check_vma=False,
    )
```

```python
import jax
import jax.numpy as jnp
from jax import lax
from jax.experimental import pallas as pl
from jax.experimental.pallas import tpu as pltpu
from jax.sharding import PartitionSpec as P

step_weight = 0.5
ridge_term = 0.01
normal_offset = 0.9189385332046727
exact_mode = lax.Precision.HIGHEST
PANEL = 32
SUB = 16
SQUARE, BOTH, START, TABLES = 0, 2, 4, 6
f32 = jnp.float32
bf16 = jnp.bfloat16


def call(body, out_shape, *args, scratch=(), flops=0, near=True):
    single = not isinstance(out_shape, (list, tuple))
    vmem = pl.BlockSpec(memory_space=pltpu.VMEM)
    hbm = pl.BlockSpec(memory_space=pltpu.HBM)
    space = pltpu.VMEM if near else pltpu.HBM
    args = [pltpu.with_memory_space_constraint(arg, space) for arg in args]
    return pl.pallas_call(
        body,
        out_shape=out_shape,
        in_specs=[vmem] * len(args),
        out_specs=vmem if single else [
            hbm if out.memory_space == pltpu.HBM else vmem for out in out_shape
        ],
        scratch_shapes=list(scratch),
        cost_estimate=pl.CostEstimate(flops=flops, transcendentals=0, bytes_accessed=0),
        compiler_params=pltpu.CompilerParams(vmem_limit_bytes=12 << 20),
    )(*args)


def place():
    return lax.axis_index("dp"), lax.axis_index("comp") % 2


def shape(dims, dtype=f32):
    return pltpu.VMEM(dims, dtype)


def far(dims, dtype=f32):
    return pltpu.HBM(dims, dtype)


def own_of(row_ref, position):
    row = row_ref[...]
    lanes = lax.broadcasted_iota(jnp.int32, row.shape, 1)
    return jnp.sum(jnp.where(lanes == position, row, 0.0), axis=1, keepdims=True)


def eye_of(size):
    rows = lax.broadcasted_iota(jnp.int32, (size, size), 0)
    cols = lax.broadcasted_iota(jnp.int32, (size, size), 1)
    return rows, cols


def three_parts(wide):
    high = wide.astype(bf16)
    rest = wide - high.astype(f32)
    mid = rest.astype(bf16)
    low = (rest - mid.astype(f32)).astype(bf16)
    return high, mid, low


def over_lanes(left, right):
    return lax.dot_general(left, right, (((1,), (1,)), ((), ())), preferred_element_type=f32)


def spread_body(vectors_ref, factors_ref, out_ref):
    unused, core = place()
    half = vectors_ref[:, pl.ds(pl.multiple_of(core * 128, 128), 128)]
    for peer in range(out_ref.shape[0]):
        out_ref[peer, :128, :] = half
        out_ref[peer, 128:144, :] = factors_ref[peer, :, :128]
        out_ref[peer, 144:160, :] = factors_ref[peer, :, 128:]


def gather_factor(got_ref, factor_ref):
    for peer in range(16):
        factor_ref[16 * peer : 16 * peer + 16, :128] = got_ref[peer, 128:144, :]
        factor_ref[16 * peer : 16 * peer + 16, 128:] = got_ref[peer, 144:160, :]


def factor_body(
    got_ref, centers_ref, mixing_ref, factor_ref, shifted_ref, constant_ref, tables_ref, inverse_ref
):
    position, unused = place()
    gather_factor(got_ref, factor_ref)
    wide = factor_ref[...].astype(f32)
    center = centers_ref[pl.ds(position, 1), :]
    shifted = jnp.sum(wide * center, axis=1, keepdims=True)
    shifted_ref[...] = jnp.broadcast_to(shifted, (256, 128))
    rows, cols = eye_of(256)
    diagonal = jnp.sum(jnp.where(rows == cols, wide, 0.0), axis=1, keepdims=True)
    log_diag = jnp.sum(jnp.log(diagonal), axis=0, keepdims=True)
    log_mix = jnp.log(own_of(mixing_ref, position))
    constant_ref[0:1, :] = jnp.broadcast_to(log_diag, (1, 128))
    constant_ref[1:2, :] = jnp.broadcast_to(log_mix, (1, 128))
    invert_body(factor_ref, tables_ref, inverse_ref)


def score_body(got_ref, other_ref, factor_ref, shifted_ref, constant_ref, out_ref, turned_ref):
    unused, core = place()
    order_body(got_ref, other_ref, turned_ref)
    mine = factor_ref[:, pl.ds(pl.multiple_of(core * 128, 128), 128)]
    rest = factor_ref[:, pl.ds(pl.multiple_of((1 - core) * 128, 128), 128)]
    for pair in range(8):
        ours = got_ref[2 * pair : 2 * pair + 2, :128, :].reshape(256, 128)
        theirs = other_ref[2 * pair : 2 * pair + 2, :128, :].reshape(256, 128)
        product = over_lanes(mine, ours) + over_lanes(rest, theirs)
        for block in range(2):
            whitened = product[:, 128 * block : 128 * block + 128] - shifted_ref[...]
            density = constant_ref[0:1, :] - 0.5 * jnp.sum(
                whitened * whitened, axis=0, keepdims=True
            )
            out_ref[2 * pair + block] = density + constant_ref[1:2, :] - 256 * normal_offset


def apart(left, right, **options):
    return jnp.dot(left, right, precision=exact_mode, preferred_element_type=f32)


def invert_body(factor_ref, tables_ref, inverse_ref):
    rows, cols = eye_of(128)
    factors = []
    for start in (0, 128):
        factor = factor_ref[start : start + 128, start : start + 128].astype(f32)
        diagonal = jnp.sum(jnp.where(rows == cols, factor, 0.0), axis=1, keepdims=True)
        factors.append(factor)
        inverse_ref[start // 128] = jnp.where(rows == cols, 1.0 / diagonal, 0.0)
    for level in range(7):
        below = (rows >> (level + 1) == cols >> (level + 1)) & (rows >> level > cols >> level)
        for block in range(2):
            inverse = inverse_ref[block]
            step = jnp.where(below, factors[block], 0.0)
            inverse_ref[block] = inverse - apart(apart(inverse, step), inverse)
    first, last = inverse_ref[0], inverse_ref[1]
    corner = -apart(apart(last, factor_ref[128:, :128].astype(f32)), first)
    bottom = jnp.concatenate([corner, last], axis=1)
    whole = jnp.concatenate(
        [jnp.concatenate([first, jnp.zeros((128, 128), f32)], axis=1), bottom], axis=0
    )
    square = lax.dot_general(
        whole, whole, (((1,), (1,)), ((), ())), precision=exact_mode, preferred_element_type=f32
    )
    rows, cols = eye_of(256)
    diagonal = jnp.where(rows == cols, square, 0.0)
    down = lax.rsqrt(1.0 + jnp.sum(diagonal, axis=1, keepdims=True))
    across = lax.rsqrt(1.0 + jnp.sum(diagonal, axis=0, keepdims=True))
    both = down * across
    tables = (square * both, both, jnp.where(rows == cols, across, 0.0))
    for place, table in zip((SQUARE, BOTH, START), tables):
        tables_ref[place] = table[:, :128]
        tables_ref[place + 1] = table[:, 128:]


INV_SCRATCH = [pltpu.VMEM((2, 128, 128), f32)]


def order_body(got_ref, other_ref, turned_ref):
    unused, core = place()
    ours = pl.ds(pl.multiple_of(core * 128, 128), 128)
    theirs = pl.ds(pl.multiple_of((1 - core) * 128, 128), 128)
    for block in range(16):
        turned_ref[block, ours, :] = got_ref[block, :128, :].T
        turned_ref[block, theirs, :] = other_ref[block, :128, :].T


def partial_body(scores_ref, out_ref):
    scores = scores_ref[:, 0, :]
    top = jnp.max(scores, axis=0, keepdims=True)
    total = jnp.sum(jnp.exp(scores - top), axis=0, keepdims=True)
    both = jnp.concatenate([top, total], axis=0)
    for peer in range(out_ref.shape[0]):
        out_ref[peer] = both


def share_body(scores_ref, pairs_ref, shares_ref, evidence_ref):
    tops, totals = pairs_ref[:, 0, :], pairs_ref[:, 1, :]
    top = jnp.max(tops, axis=0, keepdims=True)
    total = jnp.sum(totals * jnp.exp(tops - top), axis=0, keepdims=True)
    evidence_ref[...] = top + jnp.log(total)
    shares = jnp.exp(scores_ref[:, 0, :] - top) / total
    for peer in range(shares_ref.shape[0]):
        shares_ref[peer] = shares


def same_row(tile, row):
    return jnp.broadcast_to(tile[row : row + 1, :], tile.shape)


def six_products(rows):
    high, mid, low = three_parts(rows)
    turned = jnp.concatenate([high, high, mid, high, low, mid], axis=0)
    straight = jnp.concatenate([high, mid, high, low, high, mid], axis=0)
    return turned, straight


def over_rows(left, right):
    return lax.dot_general(left, right, (((0,), (0,)), ((), ())), preferred_element_type=f32)


def eliminate(start, work_ref, tables_ref, upper_ref, out_ref):
    panel, sub = PANEL, SUB
    tiles = panel // 8
    in_tile = lax.broadcasted_iota(jnp.int32, (8, 128), 0)
    lane_of = lax.broadcasted_iota(jnp.int32, (8, 128), 1)
    far_lane = lax.broadcasted_iota(jnp.int32, (1, 128), 1)
    stop = start + panel
    near = start // 128
    rows = [
        [work_ref[start + 8 * i : start + 8 * i + 8, 128 * t : 128 * t + 128] for i in range(tiles)]
        for t in range(2)
    ]
    scale = [jnp.zeros((8, 128), f32) for i in range(tiles)]
    for begin in range(0, panel, sub):
        lane = start % 128 + begin
        columns = [
            {
                i: jnp.broadcast_to(rows[near][i][:, lane + k : lane + k + 1], (8, 128))
                for i in range((begin + k) // 8, tiles)
            }
            for k in range(sub)
        ]
        cleared = (lane_of >= lane) & (lane_of < lane + sub)
        for i in range(tiles):
            fresh = tables_ref[START + near, start + 8 * i : start + 8 * i + 8, :]
            rows[near][i] = jnp.where(cleared, fresh, rows[near][i])
        for k in range(0, sub, 2):
            row = begin + k
            tile, place = row // 8, row % 8
            one, two = columns[k], columns[k + 1]
            a, b = same_row(one[tile], place), same_row(one[tile], place + 1)
            d = same_row(two[tile], place + 1)
            root = lax.rsqrt(a * d - b * b)
            inverse = root * root
            root_a = lax.rsqrt(a)
            raw = {
                i: (one[i] * d - two[i] * b, two[i] * a - one[i] * b)
                for i in range(tile, tiles)
            }
            below = in_tile > place + 1
            raw[tile] = tuple(jnp.where(below, part, 0.0) for part in raw[tile])
            ratio = {i: (raw[i][0] * inverse, raw[i][1] * inverse) for i in raw}
            for later in range(k + 2, sub):
                other = begin + later
                f = same_row(one[other // 8], other % 8)
                g = same_row(two[other // 8], other % 8)
                for i in range(other // 8, tiles):
                    if later < k + 4:
                        change = (raw[i][0] * f + raw[i][1] * g) * inverse
                    else:
                        change = ratio[i][0] * f + ratio[i][1] * g
                    columns[later][i] = columns[later][i] - change
            ratio[tile] = (
                jnp.where(in_tile == place + 1, b * (root_a * root_a), ratio[tile][0]),
                ratio[tile][1],
            )
            for group in rows:
                f, g = same_row(group[tile], place), same_row(group[tile], place + 1)
                for i in range(tile, tiles):
                    group[i] = group[i] - (ratio[i][0] * f + ratio[i][1] * g)
            scale[tile] = jnp.where(in_tile == place, root_a, scale[tile])
            scale[tile] = jnp.where(in_tile == place + 1, root * (a * root_a), scale[tile])
    solved = [
        jnp.concatenate([group[i] * scale[i] for i in range(tiles)], axis=0) for group in rows
    ]
    for t in range(2):
        lanes = slice(128 * t, 128 * t + 128)
        done = jnp.where(far_lane + 128 * t < stop, solved[t], 0.0)
        for piece in range(panel // 16):
            out_ref[start // 16 + piece, :, lanes] = done[16 * piece : 16 * piece + 16, :]
        if near == 0:
            upper_ref[start:stop, lanes] = solved[t] if t else done
    end = 128 * near + 128
    if stop == end:
        return
    turned, straight = six_products(jnp.concatenate(solved, axis=1))
    change = over_rows(turned[:, 128 * near : end], straight)
    inside = (far_lane + 128 * near >= start) & (far_lane + 128 * near < stop)
    for t in range(2):
        lanes = slice(128 * t, 128 * t + 128)
        kept = work_ref[stop:end, lanes]
        if t == near:
            kept = jnp.where(inside, 0.0, kept)
        work_ref[stop:end, lanes] = kept - change[stop - 128 * near :, lanes]


def refactor_body(
    shares_ref, turned_ref, tables_ref, centers_ref, mixing_ref,
    out_ref, means_ref, weights_ref, work_ref, upper_ref,
):
    position, unused = place()
    vector_total = turned_ref.shape[0] * turned_ref.shape[2]
    share = shares_ref[:, pl.ds(position, 1), :].reshape(16, 128)

    def weighted_parts(pair, half):
        weighted = [
            turned_ref[block, 128 * half : 128 * half + 128, :].astype(f32)
            * share[block : block + 1, :]
            for block in (2 * pair, 2 * pair + 1)
        ]
        return list(three_parts(jnp.concatenate(weighted, axis=1)))

    def vectors_of(pair, first):
        blocks = [turned_ref[block, first:, :] for block in (2 * pair, 2 * pair + 1)]
        return jnp.concatenate(blocks, axis=1)

    def added_up(parts):
        return parts[:128] + parts[128:256] + parts[256:384]

    total = jnp.zeros((432, 256), f32)
    counts = jnp.zeros((16, 128), f32)
    for pair in range(8):
        everyone = jnp.concatenate([shares_ref[2 * pair], shares_ref[2 * pair + 1]], axis=1)
        counts += everyone[:, :128] + everyone[:, 128:]
        stacked = jnp.concatenate(weighted_parts(pair, 0) + list(three_parts(everyone)), axis=0)
        total += over_lanes(stacked, vectors_of(pair, 0))
    gram = added_up(total)
    moments = total[384:400] + total[400:416] + total[416:]
    everyone_of = lax.broadcasted_iota(jnp.int32, (16, 1), 0)
    moment = jnp.sum(jnp.where(everyone_of == position, moments, 0.0), axis=0, keepdims=True)
    count = jnp.sum(jnp.sum(share, axis=0, keepdims=True), axis=1, keepdims=True)
    kept = (1.0 - step_weight) * own_of(mixing_ref, position)
    weight = kept + step_weight * count / vector_total
    center = centers_ref[pl.ds(position, 1), :]
    rows, cols = eye_of(128)
    same = rows == cols
    mean = (kept * center + step_weight * moment / vector_total) / weight

    def down(row):
        return jnp.sum(jnp.where(same, row, 0.0), axis=1, keepdims=True)

    def assembled(gram, half, t):
        mine, lanes = slice(128 * half, 128 * half + 128), slice(128 * t, 128 * t + 128)
        moment_part = (
            (kept * down(center[:, mine])) * center[:, lanes] + (step_weight / vector_total) * gram
        ) / weight - down(mean[:, mine]) * mean[:, lanes]
        if half == t:
            moment_part += jnp.where(same, ridge_term, 0.0)
        return (kept / weight) * tables_ref[SQUARE + t, mine, :] + moment_part * (
            tables_ref[BOTH + t, mine, :]
        )

    for t in range(2):
        lanes = slice(128 * t, 128 * t + 128)
        work_ref[:128, lanes] = assembled(gram[:, lanes], 0, t)
    last = jnp.zeros((384, 128), f32)
    for panel in range(128 // PANEL):
        eliminate(PANEL * panel, work_ref, tables_ref, upper_ref, out_ref)
        if panel < 2:
            for pair in range(4 * panel, 4 * panel + 4):
                stacked = jnp.concatenate(weighted_parts(pair, 1), axis=0)
                last += over_lanes(stacked, vectors_of(pair, 128))
        if panel == 0:
            few = [index[:16, :16] for index in (rows, cols)]
            everyone_at = few[0] == few[1]
            priors = jnp.sum(jnp.where(everyone_at, mixing_ref[...], 0.0), axis=1, keepdims=True)
            all_kept = (1.0 - step_weight) * priors
            counts = jnp.sum(counts, axis=1, keepdims=True)
            weights = all_kept + step_weight * counts / vector_total
            means_ref[...] = (
                all_kept * centers_ref[...] + step_weight * moments / vector_total
            ) / weights
            weights_ref[...] = jnp.sum(
                jnp.where(everyone_at, weights, 0.0), axis=0, keepdims=True
            )
        if panel == 2:
            corner = assembled(added_up(last), 1, 1)
    turned, straight = six_products(upper_ref[...])
    change = over_rows(turned[:, 128:], straight)
    work_ref[128:, :128] = -change[:, :128]
    work_ref[128:, 128:] = corner - change[:, 128:]
    for panel in range(128 // PANEL):
        eliminate(128 + PANEL * panel, work_ref, tables_ref, upper_ref, out_ref)


REF_SCRATCH = [
    pltpu.VMEM((256, 256), f32),
    pltpu.VMEM((128, 256), f32),
]


def close_body(*refs):
    sources, targets, sent_ref = refs[:4], refs[4:8], refs[8]
    copies = []
    for source, target in zip(sources[1:], targets[1:]):
        copies.append((source, target))
    for part in range(4):
        copies.append((sources[0].at[4 * part : 4 * part + 4], targets[0].at[4 * part : 4 * part + 4]))
    copies = [
        pltpu.make_async_copy(source, target, sent_ref.at[place_of])
        for place_of, (source, target) in enumerate(copies)
    ]
    for copy in copies:
        copy.start()
    for copy in copies:
        copy.wait()


def exchanged(array, axis):
    return lax.all_to_all(array, axis, split_axis=0, concat_axis=0, tiled=True)


def local(vectors, centers, factors, mixing):
    groups, peers = lax.axis_size("dp"), lax.axis_size("comp")
    priors = mixing.reshape(1, 16)
    spread = call(spread_body, shape((groups, 160, 128), bf16), vectors, factors, near=False)
    got = exchanged(spread, "dp")
    other = lax.ppermute(got, "comp", [(i, i ^ 1) for i in range(peers)])
    factor, shifted, constant, tables = call(
        factor_body,
        [shape((256, 256), bf16), shape((256, 128)), shape((2, 128)), shape((TABLES, 256, 128))],
        got, centers, priors, scratch=INV_SCRATCH, flops=1 << 27,
    )
    scores, turned = call(
        score_body, [shape((16, 1, 128)), shape((16, 256, 128), bf16)],
        got, other, factor, shifted, constant, flops=1 << 29,
    )
    scores_here = exchanged(scores, "dp")
    partial = call(partial_body, shape((peers, 2, 128)), scores_here)
    pairs = exchanged(partial, "comp")
    shares, evidence = call(
        share_body, [shape((groups, 16, 128)), shape((1, 128))], scores_here, pairs
    )
    shares_all = exchanged(shares, "dp")
    refreshed, new_means, new_weights = call(
        refactor_body, [shape((16, 16, 256)), shape((16, 256)), shape((1, 16))],
        shares_all, turned, tables, centers, priors, scratch=REF_SCRATCH, flops=1 << 32,
    )
    new_factors, new_means, new_weights, evidence = call(
        close_body, [far((16, 16, 256)), far((16, 256)), far((1, 16)), far((1, 128))],
        exchanged(refreshed, "dp"), new_means, new_weights, evidence,
        scratch=[pltpu.SemaphoreType.DMA((7,))],
    )
    return new_factors, new_means, new_weights.reshape(16), evidence.reshape(128)


def solution(mesh):
    return jax.shard_map(
        local,
        mesh=mesh,
        in_specs=(P("dp", None), P("comp", None), P("comp", "dp", None), P("comp")),
        out_specs=(P("comp", "dp", None), P("comp", None), P("comp"), P("dp")),
        check_vma=False,
    )
```
